32 devices in a mesh: node: 4 (over z), local: 8 (over y, x, core).
Axes of the slice: x: 2, y: 2, z: 4, core: 2. Of those that a mesh axis runs over, the one named last changes fastest.
Arguments:
- tokens: bfloat16 [4096, 5120], P(('node', 'local')), may hold values from -6 to 6
- routes: int32 [4096, 6], P(('node', 'local')), may hold values from 0 to 31, all different within a row; in each aligned block of 128 rows (0 to 127, 128 to 255, ...) at most 32 rows name the same one
- route_weights: float32 [4096, 6], P(('node', 'local')), may hold values from 0.05 to 1
- w_gate: bfloat16 [32, 5120, 768], P(('node', 'local')), may hold values from -0.078125 to 0.078125
- w_up: bfloat16 [32, 5120, 768], P(('node', 'local')), may hold values from -0.078125 to 0.078125
- w_down: bfloat16 [32, 768, 5120], P(('node', 'local')), may hold values from -0.21875 to 0.21875
Outputs:
- mixed: bfloat16 [4096, 5120], P(('node', 'local'))
- balance_loss: float32 [], replicated
The draws below stay inside these ranges and needn't reach their ends.
Inputs may be any that keep to these rules, and one draw needn't show every extreme that they name: `routes`: each row names 6 different experts. Among the rows of one device no expert is named more than 32 times, a bound that some block reaches.
All inputs are finite; a program needn't handle non-finite values.
Results may differ from the reference program's by a relative error of at most 0.0025.
The reference program's roundings to bfloat16 on the way count: a program that leaves them out, or rounds other values in their place, can miss the bound.
Values may be sent and summed in bfloat16 or wider, within the bound.
A program may use at most 128 MiB of HBM per device.

```python
import math
import jax
import jax.numpy as jnp
import numpy as np
from jax import lax

D = 5120
FF = 768
TOPK = 6
TOK_DEV = 128
EXPERTS = 32
TOKENS = 4096
CAP = 32
N_NODE = 4
N_LOCAL = 8


def block_scale(own_key, shape, split, least, largest):
    factor_of = 1.0
    for axis_at, shards_of in split:
        heights = jax.random.uniform(jax.random.fold_in(jax.random.fold_in(own_key, 6), axis_at), (shards_of,), jnp.float32, least / len(split), largest / len(split))
        factor_of = factor_of * jnp.repeat(jnp.exp(heights), shape[axis_at] // shards_of).reshape((-1,) + (1,) * (len(shape) - 1 - axis_at))
    return factor_of


def assign_block(key, own, number, rows, number_of, top, bound, skew):
    order = jax.random.permutation(key, number_of)
    crowded, ordinary = load_shares(number_of, rows * top, bound, skew, True), load_shares(number_of, rows * top, bound, skew, False)
    places = jnp.arange(number_of)

    def named(tallies, turn):
        used = int((tallies > 0).sum())
        fixed = max(1, used // 4)
        passed = fixed + (places - fixed + turn * (used - fixed)) % max(1, number_of - fixed)
        return jnp.zeros((number_of,), jnp.int32).at[order[jnp.where(places < fixed, places, passed)]].set(jnp.asarray(tallies, jnp.int32))

    tallies = jnp.where(number % 4 == 0, named(crowded, number // 4), named(ordinary, number - number // 4 - 1))
    mixed = jax.random.permutation(jax.random.fold_in(own, 3), number_of)
    giver, taker = mixed[0:number_of // 2 * 2:2], mixed[1:number_of // 2 * 2:2]
    room = jnp.minimum(tallies[giver] - 1, bound - tallies[taker]) // 2
    room = jnp.where((giver == order[0]) | (taker == order[0]) | (tallies[taker] == 0), 0, jnp.maximum(room, 0))
    passed = jax.random.randint(jax.random.fold_in(own, 4), (number_of // 2,), 0, 1 << 20) % (room + 1)
    tallies = tallies.at[giver].add(-passed).at[taker].add(passed)
    items = jnp.searchsorted(jnp.cumsum(tallies), jnp.arange(rows * top), side="right").astype(jnp.int32)
    table = items.reshape(top, rows).T
    table = table[jax.random.permutation(jax.random.fold_in(own, 1), rows)]
    turn = jax.random.randint(jax.random.fold_in(own, 2), (rows, 1), 0, top)
    return jnp.take_along_axis(table, (jnp.arange(top)[None, :] + turn) % top, axis=1)


def load_shares(number_of, total, bound, lean, full):
    portions = [(1 << 20) // math.isqrt(rank ** lean) + 1 for rank in range(1, number_of + 1)]
    largest = bound if full else min(bound, max(-(-total // number_of), total * portions[0] // sum(portions)))
    least = 1 if total - largest >= number_of - 1 else 0
    counts, surplus = [largest] + [least] * (number_of - 1), total - largest - least * (number_of - 1)
    while surplus > 0:
        free = [i for i in range(1, number_of) if counts[i] < largest] or [i for i in range(1, number_of) if counts[i] < bound]
        whole, remaining = sum([portions[i] for i in free]), surplus
        for i in free:
            more = min(bound - counts[i], max(1, remaining * portions[i] // whole), surplus)
            counts[i] = counts[i] + more
            surplus = surplus - more
    return np.array(counts)


def bell_draw(rng, shape, width, reach, split=(), kind=jnp.bfloat16):
    values = jax.random.normal(rng, shape, jnp.float32) * width
    if len(split) > 0:
        values = block_scale(rng, shape, split, -0.22, 0.18) * values
    return jnp.clip(values, min=-reach, max=reach).astype(kind)


def setup_inputs(seed: int = 0) -> dict:
    streams_of = jax.random.split(jax.random.key(seed), 7)
    tokens = bell_draw(streams_of[0], (TOKENS, D), 1.0, 6.0, ((0, 32),))
    routes_keys = jax.random.split(jax.random.fold_in(streams_of[1], 1), TOKENS // TOK_DEV)
    routes_turns = jax.random.permutation(jax.random.fold_in(streams_of[1], 3), TOKENS // TOK_DEV)
    routes = jax.vmap(lambda own, number: assign_block(jax.random.fold_in(streams_of[1], 2), own, number, TOK_DEV, EXPERTS, TOPK, CAP, 2))(routes_keys, routes_turns).reshape((TOKENS, TOPK))
    route_weights = jnp.clip(jnp.exp(math.log(1.0) - 2.9957323 * jax.random.uniform(streams_of[2], (TOKENS, TOPK), jnp.float32) ** block_scale(streams_of[2], (TOKENS, TOPK), ((0, 32),), -0.2, 0.2)), 0.05, 1.0)
    w_gate = bell_draw(streams_of[3], (EXPERTS, D, FF), D ** -0.5, 0.078125, ((0, 32),))
    w_up = bell_draw(streams_of[4], (EXPERTS, D, FF), D ** -0.5, 0.078125, ((0, 32),))
    w_down = bell_draw(streams_of[5], (EXPERTS, FF, D), FF ** -0.5, 0.21875, ((0, 32),))
    return {"tokens": tokens, "routes": routes, "route_weights": route_weights, "w_gate": w_gate, "w_up": w_up, "w_down": w_down}


def slots_of(flat):
    labels = jnp.arange(EXPERTS, dtype=jnp.int32)
    onehot = (flat[:, None] == labels[None, :]).astype(jnp.int32)
    running = jnp.cumsum(onehot, axis=0) - onehot
    return jnp.sum(running * onehot, axis=1).astype(jnp.int32)


def reference(tokens, routes, route_weights, w_gate, w_up, w_down):
    devices = N_NODE * N_LOCAL
    pairs = TOK_DEV * TOPK
    span = devices * CAP
    flat = routes.reshape(devices, pairs).astype(jnp.int32)
    slots = jax.vmap(slots_of)(flat)
    source = jnp.arange(devices, dtype=jnp.int32)[:, None]
    position = flat * span + source * CAP + slots
    token_ids = source * TOK_DEV + jnp.arange(pairs, dtype=jnp.int32)[None, :] // TOPK
    table = jnp.full((EXPERTS * span,), TOKENS, jnp.int32).at[position.reshape(-1)].set(token_ids.reshape(-1))
    padded = jnp.concatenate([tokens, jnp.zeros((1, D), jnp.bfloat16)], axis=0)

    def one_expert(packed):
        ids, gate_w, up_w, down_w = packed
        rows = padded[ids]
        gate = jnp.dot(rows, gate_w, preferred_element_type=jnp.float32)
        up = jnp.dot(rows, up_w, preferred_element_type=jnp.float32)
        hidden = (jax.nn.silu(gate) * up).astype(jnp.bfloat16)
        return jnp.dot(hidden, down_w, preferred_element_type=jnp.float32).astype(jnp.bfloat16)

    outputs = lax.map(one_expert, (table.reshape(EXPERTS, span), w_gate, w_up, w_down))
    outputs = outputs.reshape(EXPERTS * span, D)
    weights = route_weights.reshape(devices, TOK_DEV, TOPK)

    def one_source(packed):
        where, gates = packed
        picked = outputs[where].reshape(TOK_DEV, TOPK, D).astype(jnp.float32)
        return jnp.sum(gates[:, :, None] * picked, axis=1).astype(jnp.bfloat16)

    mixed = lax.map(one_source, (position, weights)).reshape(TOKENS, D)
    every = routes.reshape(-1).astype(jnp.int32)
    count = jax.ops.segment_sum(jnp.ones(every.shape, jnp.float32), every, num_segments=EXPERTS)
    weight_sum = jax.ops.segment_sum(route_weights.reshape(-1), every, num_segments=EXPERTS)
    total = jnp.float32(TOKENS)
    balance_loss = jnp.sum(count * weight_sum) * jnp.float32(EXPERTS) / (jnp.float32(TOPK) * total * total)
    return mixed, balance_loss
```

```python
import functools

import jax
import jax.numpy as jnp
from jax import lax
from jax.experimental import pallas as pl
from jax.experimental.pallas import tpu as pltpu
from jax.sharding import PartitionSpec as P

MESH = pl.DeviceIdType.MESH
VMEM_LIMIT = 63 * 1024 * 1024
F32, BF16, I16 = jnp.float32, jnp.bfloat16, jnp.int16
AHEAD = 2
LAG = 2


def chunks_of(width):
    return max(n for n in range(1, 11) if width % (n * 128) == 0)


def tile_of(rows):
    return max(n for n in (256, 128, 64, 32, 16, 8) if rows % n == 0)


def greet(nn, nl, mn, ml):
    barrier = pltpu.get_barrier_semaphore()
    for k in range(1, nn):
        pl.semaphore_signal(barrier, inc=1, device_id={"node": lax.rem(mn + k, nn)}, device_id_type=MESH)
    for k in range(1, nl):
        pl.semaphore_signal(barrier, inc=1, device_id={"local": lax.rem(ml + k, nl)}, device_id_type=MESH)
    pl.semaphore_wait(barrier, nn + nl - 2)


def places(info, mn, nl, topk):
    lines = info.shape[-1]
    expert = lax.broadcasted_iota(jnp.int32, (nl, lines), 0).astype(F32) + (mn * nl).astype(F32)
    named = jnp.zeros((nl, lines), F32)
    weight = jnp.zeros((nl, lines), F32)
    for k in range(topk):
        match = info[k : k + 1, :] == expert
        named = jnp.where(match, 1.0, named)
        weight = jnp.where(match, info[8 + k : 9 + k, :], weight)
    earlier = (
        lax.broadcasted_iota(jnp.int32, (lines, lines), 0) < lax.broadcasted_iota(jnp.int32, (lines, lines), 1)
    ).astype(F32)
    slot = jnp.dot(named, earlier, preferred_element_type=F32)
    return jnp.where(named > 0.0, slot, -1.0), weight


def dispatch_kernel(
    nn, nl, nch, cap, topk,
    tok, routes, gains, wg, wu,
    hid, infos_out, loss,
    held, sent, arrived, acc, wbuf, pick, turned, infos, tallies, tally,
    up_send, up_recv, dn_send, dn_recv, p_send, p_recv, i_send, i_recv, t_send, t_recv, own_sem, w_sem,
):
    mn, ml = lax.axis_index("node"), lax.axis_index("local")
    lines, width = tok.shape
    ch = width // nch
    ff = wg.shape[1]
    rows = nn * cap
    experts = nn * nl

    def cols(c):
        return pl.ds(pl.multiple_of(c * ch, 128), ch)

    def own(c):
        return pltpu.make_async_copy(tok.at[:, cols(c)], held.at[c, mn], own_sem.at[c])

    def weights(c):
        at = pl.ds(pl.multiple_of(c * ch, 128), ch)
        return (
            pltpu.make_async_copy(wg.at[at, :], wbuf.at[c, :, pl.ds(0, ff)], w_sem.at[c, 0]),
            pltpu.make_async_copy(wu.at[at, :], wbuf.at[c, :, pl.ds(ff, ff)], w_sem.at[c, 1]),
        )

    def up(c, d, block):
        return pltpu.make_async_remote_copy(
            src_ref=held.at[c, block], dst_ref=held.at[c, block],
            send_sem=up_send.at[c, d], recv_sem=up_recv.at[c, d],
            device_id={"node": mn + 1}, device_id_type=MESH,
        )

    def down(c, d, block):
        return pltpu.make_async_remote_copy(
            src_ref=held.at[c, block], dst_ref=held.at[c, block],
            send_sem=dn_send.at[c, d], recv_sem=dn_recv.at[c, d],
            device_id={"node": mn - 1}, device_id_type=MESH,
        )

    def slots_of(e):
        return pl.ds(pl.multiple_of(e * cap, cap), cap)

    def within(c, n, k):
        e = lax.rem(ml + k, nl)
        return pltpu.make_async_remote_copy(
            src_ref=sent.at[c, n, slots_of(e), :],
            dst_ref=arrived.at[c, pl.ds(pl.multiple_of(ml * rows + n * cap, cap), cap), :],
            send_sem=p_send.at[c, k - 1], recv_sem=p_recv.at[c, k - 1],
            device_id={"local": e}, device_id_type=MESH,
        )

    def within_all(c, k):
        l = lax.rem(ml + nl - k, nl)
        at = arrived.at[c, pl.ds(pl.multiple_of(l * rows, rows), rows), :]
        return pltpu.make_async_remote_copy(
            src_ref=at, dst_ref=at, send_sem=p_send.at[c, k - 1], recv_sem=p_recv.at[c, k - 1],
            device_id={"local": l}, device_id_type=MESH,
        )

    def info_copy(k):
        return pltpu.make_async_remote_copy(
            src_ref=infos.at[mn], dst_ref=infos.at[mn], send_sem=i_send.at[k - 1], recv_sem=i_recv.at[k - 1],
            device_id={"node": lax.rem(mn + k, nn)}, device_id_type=MESH,
        )

    def tally_copy(k):
        return pltpu.make_async_remote_copy(
            src_ref=tally, dst_ref=tallies.at[ml], send_sem=t_send.at[k - 1], recv_sem=t_recv.at[k - 1],
            device_id={"local": lax.rem(ml + k, nl)}, device_id_type=MESH,
        )

    def start_own(c):
        @pl.when(mn + 1 < nn)
        def _():
            up(c, 0, mn).start()

        @pl.when(mn > 0)
        def _():
            down(c, 0, mn).start()

    @pl.loop(0, nch)
    def _(c):
        own(c).start()

    @pl.loop(0, nch)
    def _(c):
        for copy in weights(c):
            copy.start()

    turned[...] = jnp.zeros(turned.shape, F32)
    named = routes[...].astype(F32)
    turned[:, 0:topk] = named
    turned[:, 8 : 8 + topk] = gains[...]
    infos[mn, 0:16, :] = turned[...].T[0:16, :]
    label = lax.broadcasted_iota(jnp.int32, (lines, tally.shape[1]), 1)
    hits = jnp.zeros(label.shape, F32)
    sums = jnp.zeros(label.shape, F32)
    for k in range(topk):
        match = routes[:, k : k + 1] == label
        hits = hits + jnp.where(match, 1.0, 0.0)
        sums = sums + jnp.where(match, gains[:, k : k + 1], 0.0)
    line = lax.broadcasted_iota(jnp.int32, (8, tally.shape[1]), 0)
    infos[mn, 16:24, :] = jnp.where(
        line == 0, jnp.sum(hits, axis=0, keepdims=True), jnp.where(line == 1, jnp.sum(sums, axis=0, keepdims=True), 0.0)
    )

    greet(nn, nl, mn, ml)
    for k in range(1, nn):
        info_copy(k).start()

    @pl.loop(0, nch)
    def _(c):
        own(c).wait()

        @pl.when(c < AHEAD)
        def _():
            start_own(c)

    def picks(n):
        slot, _ = places(infos[n], mn, nl, topk)
        rank = lax.broadcasted_iota(jnp.int32, (cap, lines), 0).astype(F32)
        for e in range(nl):
            pick[n, e * cap : (e + 1) * cap, :] = jnp.where(slot[e : e + 1, :] == rank, 1.0, 0.0).astype(BF16)

    def hand_out(c, n):
        picked = jnp.dot(pick[n], held[c, n], preferred_element_type=F32)
        sent[c, n] = picked.astype(BF16)
        for k in range(1, nl):
            within(c, n, k).start()
        arrived[c, pl.ds(pl.multiple_of(ml * rows + n * cap, cap), cap), :] = sent[c, n, slots_of(ml), :]

    picks(mn)

    @pl.loop(0, nch)
    def _(c):
        hand_out(c, mn)

    for k in range(1, nn):
        info_copy(k).wait_recv()
    total = infos[0, 16:24, :]
    for n in range(1, nn):
        total = total + infos[n, 16:24, :]
    tally[...] = total
    tallies[ml] = total
    for k in range(1, nl):
        tally_copy(k).start()

    @pl.loop(0, nn)
    def _(n):
        @pl.when(n != mn)
        def _():
            picks(n)

    acc[...] = jnp.zeros(acc.shape, F32)
    step = tile_of(nl * rows)

    def multiply(c):
        for copy in weights(c):
            copy.wait()
        for k in range(1, nl):
            within_all(c, k).wait_recv()

        @pl.loop(0, nl * rows // step)
        def _(m):
            at = pl.ds(pl.multiple_of(m * step, step), step)
            acc[at, :] += jnp.dot(arrived[c, at, :], wbuf[c], preferred_element_type=F32)

    @pl.loop(0, nch + LAG)
    def _(i):
        @pl.when(i < nch)
        def _():
            @pl.when(i + AHEAD < nch)
            def _():
                start_own(i + AHEAD)

            for d in range(nn - 1):
                @pl.when(mn - 1 - d >= 0)
                def _():
                    block = mn - 1 - d
                    up(i, d, block).wait_recv()

                    if d + 1 < nn - 1:
                        @pl.when(mn + 1 < nn)
                        def _():
                            up(i, d + 1, block).start()

                @pl.when(mn + 1 + d < nn)
                def _():
                    block = mn + 1 + d
                    down(i, d, block).wait_recv()

                    if d + 1 < nn - 1:
                        @pl.when(mn > 0)
                        def _():
                            down(i, d + 1, block).start()

            @pl.loop(0, nn)
            def _(n):
                @pl.when(n != mn)
                def _():
                    hand_out(i, n)

        @pl.when(i >= LAG)
        def _():
            multiply(i - LAG)

    @pl.loop(0, nl * rows // step)
    def _(m):
        at = pl.ds(pl.multiple_of(m * step, step), step)
        gate = acc[at, 0:ff]
        hid[at, :] = (gate / (1.0 + jnp.exp(-gate)) * acc[at, ff : 2 * ff]).astype(BF16)

    infos_out[...] = infos[...]
    for k in range(1, nl):
        tally_copy(k).wait_recv()
    total = tallies[0]
    for l in range(1, nl):
        total = total + tallies[l]
    tokens = float(lines * experts)
    loss[...] = jnp.sum(total[0:1, :] * total[1:2, :], axis=1, keepdims=True) * (experts / (topk * tokens * tokens))

    for k in range(1, nn):
        info_copy(k).wait_send()
    for k in range(1, nl):
        tally_copy(k).wait_send()

    @pl.loop(0, nch)
    def _(c):
        for k in range(1, nl):
            within_all(c, k).wait_send()
        for d in range(nn - 1):
            @pl.when((mn + 1 < nn) & (mn - d >= 0))
            def _():
                up(c, d, mn - d).wait_send()

            @pl.when((mn > 0) & (mn + d < nn))
            def _():
                down(c, d, mn + d).wait_send()


def return_kernel(
    nn, nl, nch, cap, topk,
    hid, infos, wd,
    out,
    wbuf, y, held, mix, part, scale, base, got, got_scale,
    p_send, p_recv, z_send, z_recv, s_send, s_recv, w_sem,
):
    mn, ml = lax.axis_index("node"), lax.axis_index("local")
    lines, width = out.shape
    ch = width // nch
    rows = nn * cap
    step = tile_of(nl * rows)

    def cols(c):
        return pl.ds(pl.multiple_of(c * ch, 128), ch)

    def weights(c):
        return pltpu.make_async_copy(wd.at[:, cols(c)], wbuf.at[c], w_sem.at[c])

    def slots_of(e):
        return pl.ds(pl.multiple_of(e * cap, cap), cap)

    def within(c, n, k):
        l = lax.rem(ml + k, nl)
        return pltpu.make_async_remote_copy(
            src_ref=y.at[c, pl.ds(pl.multiple_of(l * rows + n * cap, cap), cap), :],
            dst_ref=held.at[c, n, slots_of(ml), :],
            send_sem=p_send.at[c, k - 1], recv_sem=p_recv.at[c, k - 1],
            device_id={"local": l}, device_id_type=MESH,
        )

    def within_all(c, k):
        l = lax.rem(ml + k, nl)
        at = y.at[c, pl.ds(pl.multiple_of(l * rows, rows), rows), :]
        return pltpu.make_async_remote_copy(
            src_ref=at, dst_ref=at, send_sem=p_send.at[c, k - 1], recv_sem=p_recv.at[c, k - 1],
            device_id={"local": l}, device_id_type=MESH,
        )

    def along(c, k):
        p = lax.rem(mn + k, nn)
        return (
            pltpu.make_async_remote_copy(
                src_ref=part.at[c, k - 1], dst_ref=got.at[c, k - 1],
                send_sem=z_send.at[c, k - 1], recv_sem=z_recv.at[c, k - 1],
                device_id={"node": p}, device_id_type=MESH,
            ),
            pltpu.make_async_remote_copy(
                src_ref=scale.at[c, k - 1], dst_ref=got_scale.at[c, k - 1],
                send_sem=s_send.at[c, k - 1], recv_sem=s_recv.at[c, k - 1],
                device_id={"node": p}, device_id_type=MESH,
            ),
        )

    @pl.loop(0, nch)
    def _(c):
        weights(c).start()

    greet(nn, nl, mn, ml)

    @pl.loop(0, nch)
    def _(c):
        weights(c).wait()

        @pl.loop(0, nl * rows // step)
        def _(m):
            at = pl.ds(pl.multiple_of(m * step, step), step)
            y[c, at, :] = jnp.dot(hid[at, :], wbuf[c], preferred_element_type=F32).astype(BF16)

        for k in range(1, nl):
            for n in range(nn):
                within(c, n, k).start()
        for n in range(nn):
            held[c, n, slots_of(ml), :] = y[c, pl.ds(pl.multiple_of(ml * rows + n * cap, cap), cap), :]

    @pl.loop(0, nn)
    def _(n):
        slot, weight = places(infos[n], mn, nl, topk)
        rank = lax.broadcasted_iota(jnp.int32, (cap, lines), 0).astype(F32)
        back = jnp.concatenate(
            [jnp.where(slot[e : e + 1, :] == rank, weight[e : e + 1, :], 0.0) for e in range(nl)], axis=0
        ).T
        high = back.astype(BF16)
        rest = back - high.astype(F32)
        middle = rest.astype(BF16)
        low = (rest - middle.astype(F32)).astype(BF16)
        mix[n, 0:lines, :] = high
        mix[n, lines : 2 * lines, :] = middle
        mix[n, 2 * lines : 3 * lines, :] = low

    diagonal = lax.broadcasted_iota(jnp.int32, (lines, lines), 0) == lax.broadcasted_iota(jnp.int32, (lines, lines), 1)

    def blend(c, n):
        terms = jnp.dot(mix[n], held[c, n], preferred_element_type=F32)
        return terms[0:lines] + terms[lines : 2 * lines] + terms[2 * lines : 3 * lines]

    @pl.loop(0, nch)
    def _(c):
        for k in range(1, nl):
            within_all(c, k).wait_recv()
        for k in range(1, nn):
            value = blend(c, lax.rem(mn + k, nn))
            peak = jnp.maximum(jnp.max(jnp.abs(value), axis=1, keepdims=True), 1e-30)
            part[c, k - 1] = jnp.round(value * (32767.0 / peak)).astype(jnp.int32).astype(I16)
            scale[c, k - 1] = jnp.broadcast_to(
                jnp.sum(jnp.where(diagonal, peak, 0.0), axis=0, keepdims=True), (8, lines)
            )
            for copy in along(c, k):
                copy.start()
        base[c] = blend(c, mn)

    @pl.loop(0, nch)
    def _(c):
        total = base[c]
        for k in range(1, nn):
            for copy in along(c, k):
                copy.wait_recv()
            peak = jnp.sum(jnp.where(diagonal, got_scale[c, k - 1, 0:1, :], 0.0), axis=1, keepdims=True)
            total = total + got[c, k - 1].astype(jnp.int32).astype(F32) * (peak * (1.0 / 32767.0))
        out[:, cols(c)] = total.astype(out.dtype)
        for k in range(1, nl):
            within_all(c, k).wait_send()
        for k in range(1, nn):
            for copy in along(c, k):
                copy.wait_send()


def sems(*shape):
    return pltpu.SemaphoreType.DMA(shape)


def local(tokens, routes, route_weights, w_gate, w_up, w_down):
    nn, nl = lax.axis_size("node"), lax.axis_size("local")
    exp_dev, width, ff = w_gate.shape
    experts = exp_dev * nn * nl
    assert exp_dev == 1
    lines, topk = routes.shape
    assert topk <= 8
    cap = 4 * lines * topk // (3 * experts)
    rows = nn * cap
    nch = chunks_of(width)
    ch = width // nch
    wide = -(-experts // 128) * 128
    assert wide == lines

    vmem = pl.BlockSpec(memory_space=pltpu.VMEM)
    hbm = pl.BlockSpec(memory_space=pl.ANY)
    hidden, infos, loss = pl.pallas_call(
        functools.partial(dispatch_kernel, nn, nl, nch, cap, topk),
        out_shape=(
            jax.ShapeDtypeStruct((nl * rows, ff), BF16),
            jax.ShapeDtypeStruct((nn, 24, lines), F32),
            jax.ShapeDtypeStruct((1, 1), F32),
        ),
        in_specs=[hbm, vmem, vmem, hbm, hbm],
        out_specs=(vmem, vmem, vmem),
        scratch_shapes=[
            pltpu.VMEM((nch, nn, lines, ch), BF16),
            pltpu.VMEM((nch, nn, nl * cap, ch), BF16),
            pltpu.VMEM((nch, nl * rows, ch), BF16),
            pltpu.VMEM((nl * rows, 2 * ff), F32),
            pltpu.VMEM((nch, ch, 2 * ff), BF16),
            pltpu.VMEM((nn, nl * cap, lines), BF16),
            pltpu.VMEM((lines, 128), F32),
            pltpu.VMEM((nn, 24, lines), F32),
            pltpu.VMEM((nl, 8, wide), F32),
            pltpu.VMEM((8, wide), F32),
            sems(nch, nn - 1), sems(nch, nn - 1), sems(nch, nn - 1), sems(nch, nn - 1),
            sems(nch, nl - 1), sems(nch, nl - 1),
            sems(nn - 1), sems(nn - 1), sems(nl - 1), sems(nl - 1),
            sems(nch), sems(nch, 2),
        ],
        compiler_params=pltpu.CompilerParams(collective_id=0, has_side_effects=True, vmem_limit_bytes=VMEM_LIMIT),
    )(tokens, routes, route_weights, w_gate[0], w_up[0])

    mixed = pl.pallas_call(
        functools.partial(return_kernel, nn, nl, nch, cap, topk),
        out_shape=jax.ShapeDtypeStruct((lines, width), tokens.dtype),
        in_specs=[vmem, vmem, hbm],
        out_specs=vmem,
        scratch_shapes=[
            pltpu.VMEM((nch, ff, ch), BF16),
            pltpu.VMEM((nch, nl * rows, ch), BF16),
            pltpu.VMEM((nch, nn, nl * cap, ch), BF16),
            pltpu.VMEM((nn, 3 * lines, nl * cap), BF16),
            pltpu.VMEM((nch, nn - 1, lines, ch), I16),
            pltpu.VMEM((nch, nn - 1, 8, lines), F32),
            pltpu.VMEM((nch, lines, ch), F32),
            pltpu.VMEM((nch, nn - 1, lines, ch), I16),
            pltpu.VMEM((nch, nn - 1, 8, lines), F32),
            sems(nch, nl - 1), sems(nch, nl - 1),
            sems(nch, nn - 1), sems(nch, nn - 1), sems(nch, nn - 1), sems(nch, nn - 1),
            sems(nch),
        ],
        compiler_params=pltpu.CompilerParams(collective_id=1, has_side_effects=True, vmem_limit_bytes=VMEM_LIMIT),
    )(hidden, infos, w_down[0])
    return (mixed, loss.reshape(()))


def solution(mesh):
    placed = (
        P(("node", "local"), None),
        P(("node", "local"), None),
        P(("node", "local"), None),
        P(("node", "local"), None, None),
        P(("node", "local"), None, None),
        P(("node", "local"), None, None),
    )
    return jax.shard_map(
        local,
        mesh=mesh,
        in_specs=placed,
        out_specs=(P(("node", "local"), None), P()),
        check_vma=False,
    )
```

```python
import functools

import jax
import jax.numpy as jnp
from jax import lax
from jax.experimental import pallas as pl
from jax.experimental.pallas import tpu as pltpu
from jax.sharding import PartitionSpec as P

MESH = pl.DeviceIdType.MESH
VMEM_LIMIT = 63 * 1024 * 1024
F32, BF16, I16 = jnp.float32, jnp.bfloat16, jnp.int16
AHEAD = 2
LAG = 2


def chunks_of(width):
    return max(n for n in range(1, 11) if width % (n * 128) == 0)


def tile_of(rows):
    return max(n for n in (256, 128, 64, 32, 16, 8) if rows % n == 0)


def greet(nn, nl, mn, ml):
    barrier = pltpu.get_barrier_semaphore()
    for k in range(1, nn):
        pl.semaphore_signal(barrier, inc=1, device_id={"node": lax.rem(mn + k, nn)}, device_id_type=MESH)
    for k in range(1, nl):
        pl.semaphore_signal(barrier, inc=1, device_id={"local": lax.rem(ml + k, nl)}, device_id_type=MESH)
    pl.semaphore_wait(barrier, nn + nl - 2)


def places(info, mn, nl, topk):
    lines = info.shape[-1]
    expert = lax.broadcasted_iota(jnp.int32, (nl, lines), 0).astype(F32) + (mn * nl).astype(F32)
    named = jnp.zeros((nl, lines), F32)
    weight = jnp.zeros((nl, lines), F32)
    for k in range(topk):
        match = info[k : k + 1, :] == expert
        named = jnp.where(match, 1.0, named)
        weight = jnp.where(match, info[8 + k : 9 + k, :], weight)
    earlier = (
        lax.broadcasted_iota(jnp.int32, (lines, lines), 0) < lax.broadcasted_iota(jnp.int32, (lines, lines), 1)
    ).astype(F32)
    slot = jnp.dot(named, earlier, preferred_element_type=F32)
    return jnp.where(named > 0.0, slot, -1.0), weight


def dispatch_kernel(
    nn, nl, nch, cap, topk,
    tok, routes, gains, wg, wu,
    hid, infos_out, loss,
    held, sent, arrived, acc, wbuf, pick, infos, tallies, tally,
    up_send, up_recv, dn_send, dn_recv, p_send, p_recv, i_send, i_recv, t_send, t_recv, own_sem, w_sem,
):
    mn, ml = lax.axis_index("node"), lax.axis_index("local")
    lines, width = tok.shape
    ch = width // nch
    ff = wg.shape[1]
    rows = nn * cap
    experts = nn * nl

    def cols(c):
        return pl.ds(pl.multiple_of(c * ch, 128), ch)

    def own(c):
        return pltpu.make_async_copy(tok.at[:, cols(c)], held.at[c, mn], own_sem.at[c])

    def weights(c):
        at = pl.ds(pl.multiple_of(c * ch, 128), ch)
        return (
            pltpu.make_async_copy(wg.at[at, :], wbuf.at[c, :, pl.ds(0, ff)], w_sem.at[c, 0]),
            pltpu.make_async_copy(wu.at[at, :], wbuf.at[c, :, pl.ds(ff, ff)], w_sem.at[c, 1]),
        )

    def up(c, d, block):
        return pltpu.make_async_remote_copy(
            src_ref=held.at[c, block], dst_ref=held.at[c, block],
            send_sem=up_send.at[c, d], recv_sem=up_recv.at[c, d],
            device_id={"node": mn + 1}, device_id_type=MESH,
        )

    def down(c, d, block):
        return pltpu.make_async_remote_copy(
            src_ref=held.at[c, block], dst_ref=held.at[c, block],
            send_sem=dn_send.at[c, d], recv_sem=dn_recv.at[c, d],
            device_id={"node": mn - 1}, device_id_type=MESH,
        )

    def slots_of(e):
        return pl.ds(pl.multiple_of(e * cap, cap), cap)

    def within(c, n, k):
        e = lax.rem(ml + k, nl)
        return pltpu.make_async_remote_copy(
            src_ref=sent.at[c, n, slots_of(e), :],
            dst_ref=arrived.at[c, pl.ds(pl.multiple_of(ml * rows + n * cap, cap), cap), :],
            send_sem=p_send.at[c, k - 1], recv_sem=p_recv.at[c, k - 1],
            device_id={"local": e}, device_id_type=MESH,
        )

    def within_all(c, k):
        l = lax.rem(ml + nl - k, nl)
        at = arrived.at[c, pl.ds(pl.multiple_of(l * rows, rows), rows), :]
        return pltpu.make_async_remote_copy(
            src_ref=at, dst_ref=at, send_sem=p_send.at[c, k - 1], recv_sem=p_recv.at[c, k - 1],
            device_id={"local": l}, device_id_type=MESH,
        )

    def info_copy(k):
        return pltpu.make_async_remote_copy(
            src_ref=infos.at[mn], dst_ref=infos.at[mn], send_sem=i_send.at[k - 1], recv_sem=i_recv.at[k - 1],
            device_id={"node": lax.rem(mn + k, nn)}, device_id_type=MESH,
        )

    def tally_copy(k):
        return pltpu.make_async_remote_copy(
            src_ref=tally, dst_ref=tallies.at[ml], send_sem=t_send.at[k - 1], recv_sem=t_recv.at[k - 1],
            device_id={"local": lax.rem(ml + k, nl)}, device_id_type=MESH,
        )

    def start_own(c):
        @pl.when(mn + 1 < nn)
        def _():
            up(c, 0, mn).start()

        @pl.when(mn > 0)
        def _():
            down(c, 0, mn).start()

    @pl.loop(0, nch)
    def _(c):
        own(c).start()

    @pl.loop(0, nch)
    def _(c):
        for copy in weights(c):
            copy.start()

    infos[mn, 0:16, :] = jnp.zeros((16, lines), F32)
    infos[mn, 0:topk, :] = routes[...].astype(F32)
    infos[mn, 8 : 8 + topk, :] = gains[...]
    label = lax.broadcasted_iota(jnp.int32, (tally.shape[1], lines), 0)
    hits = jnp.zeros(label.shape, F32)
    sums = jnp.zeros(label.shape, F32)
    for k in range(topk):
        match = routes[k : k + 1, :] == label
        hits = jnp.where(match, 1.0, hits)
        sums = jnp.where(match, gains[k : k + 1, :], sums)
    line = lax.broadcasted_iota(jnp.int32, (8, tally.shape[1]), 0)
    infos[mn, 16:24, :] = jnp.where(
        line == 0,
        jnp.sum(hits.T, axis=0, keepdims=True),
        jnp.where(line == 1, jnp.sum(sums.T, axis=0, keepdims=True), 0.0),
    )

    greet(nn, nl, mn, ml)
    for k in range(1, nn):
        info_copy(k).start()

    @pl.loop(0, nch)
    def _(c):
        own(c).wait()

        @pl.when(c < AHEAD)
        def _():
            start_own(c)

    def picks(n):
        slot, _ = places(infos[n], mn, nl, topk)
        rank = lax.broadcasted_iota(jnp.int32, (cap, lines), 0).astype(F32)
        for e in range(nl):
            pick[n, e * cap : (e + 1) * cap, :] = jnp.where(slot[e : e + 1, :] == rank, 1.0, 0.0).astype(BF16)

    def hand_out(c, n):
        picked = jnp.dot(pick[n], held[c, n], preferred_element_type=F32)
        sent[c, n] = picked.astype(BF16)
        for k in range(1, nl):
            within(c, n, k).start()
        arrived[c, pl.ds(pl.multiple_of(ml * rows + n * cap, cap), cap), :] = sent[c, n, slots_of(ml), :]

    picks(mn)

    @pl.loop(0, nch)
    def _(c):
        hand_out(c, mn)

    for k in range(1, nn):
        info_copy(k).wait_recv()
    total = infos[0, 16:24, :]
    for n in range(1, nn):
        total = total + infos[n, 16:24, :]
    tally[...] = total
    tallies[ml] = total
    for k in range(1, nl):
        tally_copy(k).start()

    @pl.loop(0, nn)
    def _(n):
        @pl.when(n != mn)
        def _():
            picks(n)

    acc[...] = jnp.zeros(acc.shape, F32)
    step = tile_of(nl * rows)

    def multiply(c):
        for copy in weights(c):
            copy.wait()
        for k in range(1, nl):
            within_all(c, k).wait_recv()

        @pl.loop(0, nl * rows // step)
        def _(m):
            at = pl.ds(pl.multiple_of(m * step, step), step)
            acc[at, :] += jnp.dot(arrived[c, at, :], wbuf[c], preferred_element_type=F32)

    @pl.loop(0, nch + LAG)
    def _(i):
        @pl.when(i < nch)
        def _():
            @pl.when(i + AHEAD < nch)
            def _():
                start_own(i + AHEAD)

            for d in range(nn - 1):
                @pl.when(mn - 1 - d >= 0)
                def _():
                    block = mn - 1 - d
                    up(i, d, block).wait_recv()

                    if d + 1 < nn - 1:
                        @pl.when(mn + 1 < nn)
                        def _():
                            up(i, d + 1, block).start()

                @pl.when(mn + 1 + d < nn)
                def _():
                    block = mn + 1 + d
                    down(i, d, block).wait_recv()

                    if d + 1 < nn - 1:
                        @pl.when(mn > 0)
                        def _():
                            down(i, d + 1, block).start()

            @pl.loop(0, nn)
            def _(n):
                @pl.when(n != mn)
                def _():
                    hand_out(i, n)

        @pl.when(i >= LAG)
        def _():
            multiply(i - LAG)

    @pl.loop(0, nl * rows // step)
    def _(m):
        at = pl.ds(pl.multiple_of(m * step, step), step)
        gate = acc[at, 0:ff]
        hid[at, :] = (gate / (1.0 + jnp.exp(-gate)) * acc[at, ff : 2 * ff]).astype(BF16)

    infos_out[...] = infos[...]
    for k in range(1, nl):
        tally_copy(k).wait_recv()
    total = tallies[0]
    for l in range(1, nl):
        total = total + tallies[l]
    tokens = float(lines * experts)
    loss[...] = jnp.sum(total[0:1, :] * total[1:2, :], axis=1, keepdims=True) * (experts / (topk * tokens * tokens))

    for k in range(1, nn):
        info_copy(k).wait_send()
    for k in range(1, nl):
        tally_copy(k).wait_send()

    @pl.loop(0, nch)
    def _(c):
        for k in range(1, nl):
            within_all(c, k).wait_send()
        for d in range(nn - 1):
            @pl.when((mn + 1 < nn) & (mn - d >= 0))
            def _():
                up(c, d, mn - d).wait_send()

            @pl.when((mn > 0) & (mn + d < nn))
            def _():
                down(c, d, mn + d).wait_send()


def return_kernel(
    nn, nl, nch, cap, topk,
    hid, infos, wd,
    out,
    wbuf, y, held, mix, work, part, scale, got, got_scale,
    p_send, p_recv, o_send, o_recv, z_send, z_recv, s_send, s_recv, w_sem,
):
    mn, ml = lax.axis_index("node"), lax.axis_index("local")
    lines, width = out.shape
    ch = width // nch
    rows = nn * cap
    step = tile_of(nl * rows)

    def cols(c):
        return pl.ds(pl.multiple_of(c * ch, 128), ch)

    def weights(c):
        return pltpu.make_async_copy(wd.at[:, cols(c)], wbuf.at[c], w_sem.at[c])

    def slots_of(e):
        return pl.ds(pl.multiple_of(e * cap, cap), cap)

    def within(c, n, k, send, recv):
        l = lax.rem(ml + k, nl)
        return pltpu.make_async_remote_copy(
            src_ref=y.at[c, pl.ds(pl.multiple_of(l * rows + n * cap, cap), cap), :],
            dst_ref=held.at[c, n, slots_of(ml), :],
            send_sem=send.at[c, k - 1], recv_sem=recv.at[c, k - 1],
            device_id={"local": l}, device_id_type=MESH,
        )

    def within_far(c, k):
        at = y.at[c, pl.ds(0, rows - cap), :]
        return pltpu.make_async_remote_copy(
            src_ref=at, dst_ref=at, send_sem=p_send.at[c, k - 1], recv_sem=p_recv.at[c, k - 1],
            device_id={"local": lax.rem(ml + k, nl)}, device_id_type=MESH,
        )

    def along(c, p, toward):
        mine = jnp.where(p < mn, p, p - 1)
        there = jnp.where(p > mn, p, jnp.where(p == mn - 1, nn, p))
        return (
            pltpu.make_async_remote_copy(
                src_ref=part.at[c, mine], dst_ref=got.at[c, there],
                send_sem=z_send.at[c, mine], recv_sem=z_recv.at[c, there],
                device_id={"node": mn + toward}, device_id_type=MESH,
            ),
            pltpu.make_async_remote_copy(
                src_ref=scale.at[c, mine], dst_ref=got_scale.at[c, there],
                send_sem=s_send.at[c, mine], recv_sem=s_recv.at[c, there],
                device_id={"node": mn + toward}, device_id_type=MESH,
            ),
        )

    def land(c, slot, toward):
        for buffer, sem in ((got, z_recv), (got_scale, s_recv)):
            pltpu.make_async_remote_copy(
                src_ref=buffer.at[c, slot], dst_ref=buffer.at[c, slot],
                send_sem=sem.at[c, slot], recv_sem=sem.at[c, slot],
                device_id={"node": mn - toward}, device_id_type=MESH,
            ).wait_recv()

    @pl.loop(0, nch)
    def _(c):
        weights(c).start()

    greet(nn, nl, mn, ml)

    @pl.loop(0, nch)
    def _(c):
        weights(c).wait()

        @pl.loop(0, nl * rows // step)
        def _(m):
            at = pl.ds(pl.multiple_of(m * step, step), step)
            y[c, at, :] = jnp.dot(hid[at, :], wbuf[c], preferred_element_type=F32).astype(BF16)

        for k in range(1, nl):
            for j in range(1, nn):
                within(c, lax.rem(mn + j, nn), k, p_send, p_recv).start()
        for n in range(nn):
            held[c, n, slots_of(ml), :] = y[c, pl.ds(pl.multiple_of(ml * rows + n * cap, cap), cap), :]

    @pl.loop(0, nch)
    def _(c):
        for k in range(1, nl):
            within(c, mn, k, o_send, o_recv).start()

    @pl.loop(0, nn)
    def _(n):
        slot, weight = places(infos[n], mn, nl, topk)
        rank = lax.broadcasted_iota(jnp.int32, (cap, lines), 0).astype(F32)
        back = jnp.concatenate(
            [jnp.where(slot[e : e + 1, :] == rank, weight[e : e + 1, :], 0.0) for e in range(nl)], axis=0
        ).T
        high = back.astype(BF16)
        rest = back - high.astype(F32)
        middle = rest.astype(BF16)
        low = (rest - middle.astype(F32)).astype(BF16)
        mix[n, 0:lines, :] = high
        mix[n, lines : 2 * lines, :] = middle
        mix[n, 2 * lines : 3 * lines, :] = low

    diagonal = lax.broadcasted_iota(jnp.int32, (lines, lines), 0) == lax.broadcasted_iota(jnp.int32, (lines, lines), 1)

    def blend(c, n):
        terms = jnp.dot(mix[n], held[c, n], preferred_element_type=F32)
        return terms[0:lines] + terms[lines : 2 * lines] + terms[2 * lines : 3 * lines]

    def widened(c, slot):
        peak = jnp.sum(jnp.where(diagonal, got_scale[c, slot, 0:1, :], 0.0), axis=1, keepdims=True)
        return got[c, slot].astype(jnp.int32).astype(F32) * (peak * (1.0 / 32767.0))

    def pass_on(c, p, toward, relay):
        work[...] = blend(c, p)

        @pl.when(relay)
        def _():
            land(c, p, toward)
            work[...] += widened(c, p)

        value = work[...]
        peak = jnp.maximum(jnp.max(jnp.abs(value), axis=1, keepdims=True), 1e-30)
        mine = jnp.where(p < mn, p, p - 1)
        part[c, mine] = jnp.round(value * (32767.0 / peak)).astype(jnp.int32).astype(I16)
        scale[c, mine] = jnp.broadcast_to(jnp.sum(jnp.where(diagonal, peak, 0.0), axis=0, keepdims=True), (8, lines))
        for copy in along(c, p, toward):
            copy.start()

    @pl.loop(0, nch + nn - 2)
    def _(i):
        @pl.when(i < nch)
        def _():
            for k in range(1, nl):
                within_far(i, k).wait_recv()

        c_up = i - mn
        c_down = i - (nn - 1 - mn)
        for d in reversed(range(nn - 1)):
            @pl.when((c_up >= 0) & (c_up < nch) & (mn + 1 + d < nn))
            def _():
                pass_on(c_up, mn + 1 + d, 1, mn > 0)

            @pl.when((c_down >= 0) & (c_down < nch) & (mn - 1 - d >= 0))
            def _():
                pass_on(c_down, mn - 1 - d, -1, mn < nn - 1)

    @pl.loop(0, nch)
    def _(c):
        for k in range(1, nl):
            within(c, mn, k, o_send, o_recv).wait_recv()
        work[...] = blend(c, mn)

        @pl.when(mn > 0)
        def _():
            land(c, mn, 1)
            work[...] += widened(c, mn)

        @pl.when(mn < nn - 1)
        def _():
            land(c, nn, -1)
            work[...] += widened(c, nn)

        out[:, cols(c)] = work[...].astype(out.dtype)

    @pl.loop(0, nch)
    def _(c):
        for k in range(1, nl):
            within_far(c, k).wait_send()
            within(c, mn, k, o_send, o_recv).wait_send()
        for d in range(nn - 1):
            @pl.when(mn + 1 + d < nn)
            def _():
                for copy in along(c, mn + 1 + d, 1):
                    copy.wait_send()

            @pl.when(mn - 1 - d >= 0)
            def _():
                for copy in along(c, mn - 1 - d, -1):
                    copy.wait_send()


def sems(*shape):
    return pltpu.SemaphoreType.DMA(shape)


def local(tokens, routes, route_weights, w_gate, w_up, w_down):
    nn, nl = lax.axis_size("node"), lax.axis_size("local")
    exp_dev, width, ff = w_gate.shape
    experts = exp_dev * nn * nl
    assert exp_dev == 1
    lines, topk = routes.shape
    assert topk <= 8
    cap = 4 * lines * topk // (3 * experts)
    rows = nn * cap
    nch = chunks_of(width)
    ch = width // nch
    wide = -(-experts // 128) * 128
    assert wide == lines

    vmem = pl.BlockSpec(memory_space=pltpu.VMEM)
    hbm = pl.BlockSpec(memory_space=pl.ANY)
    hidden, infos, loss = pl.pallas_call(
        functools.partial(dispatch_kernel, nn, nl, nch, cap, topk),
        out_shape=(
            jax.ShapeDtypeStruct((nl * rows, ff), BF16),
            jax.ShapeDtypeStruct((nn, 24, lines), F32),
            jax.ShapeDtypeStruct((1, 1), F32),
        ),
        in_specs=[hbm, vmem, vmem, hbm, hbm],
        out_specs=(vmem, vmem, vmem),
        scratch_shapes=[
            pltpu.VMEM((nch, nn, lines, ch), BF16),
            pltpu.VMEM((nch, nn, nl * cap, ch), BF16),
            pltpu.VMEM((nch, nl * rows, ch), BF16),
            pltpu.VMEM((nl * rows, 2 * ff), F32),
            pltpu.VMEM((nch, ch, 2 * ff), BF16),
            pltpu.VMEM((nn, nl * cap, lines), BF16),
            pltpu.VMEM((nn, 24, lines), F32),
            pltpu.VMEM((nl, 8, wide), F32),
            pltpu.VMEM((8, wide), F32),
            sems(nch, nn - 1), sems(nch, nn - 1), sems(nch, nn - 1), sems(nch, nn - 1),
            sems(nch, nl - 1), sems(nch, nl - 1),
            sems(nn - 1), sems(nn - 1), sems(nl - 1), sems(nl - 1),
            sems(nch), sems(nch, 2),
        ],
        compiler_params=pltpu.CompilerParams(collective_id=0, has_side_effects=True, vmem_limit_bytes=VMEM_LIMIT),
    )(tokens, routes.T, route_weights.T, w_gate[0], w_up[0])

    mixed = pl.pallas_call(
        functools.partial(return_kernel, nn, nl, nch, cap, topk),
        out_shape=jax.ShapeDtypeStruct((lines, width), tokens.dtype),
        in_specs=[vmem, vmem, hbm],
        out_specs=vmem,
        scratch_shapes=[
            pltpu.VMEM((nch, ff, ch), BF16),
            pltpu.VMEM((nch, nl * rows, ch), BF16),
            pltpu.VMEM((nch, nn, nl * cap, ch), BF16),
            pltpu.VMEM((nn, 3 * lines, nl * cap), BF16),
            pltpu.VMEM((lines, ch), F32),
            pltpu.VMEM((nch, nn - 1, lines, ch), I16),
            pltpu.VMEM((nch, nn - 1, 8, lines), F32),
            pltpu.VMEM((nch, nn + 1, lines, ch), I16),
            pltpu.VMEM((nch, nn + 1, 8, lines), F32),
            sems(nch, nl - 1), sems(nch, nl - 1), sems(nch, nl - 1), sems(nch, nl - 1),
            sems(nch, nn - 1), sems(nch, nn + 1), sems(nch, nn - 1), sems(nch, nn + 1),
            sems(nch),
        ],
        compiler_params=pltpu.CompilerParams(collective_id=1, has_side_effects=True, vmem_limit_bytes=VMEM_LIMIT),
    )(hidden, infos, w_down[0])
    return (mixed, loss.reshape(()))


def solution(mesh):
    placed = (
        P(("node", "local"), None),
        P(("node", "local"), None),
        P(("node", "local"), None),
        P(("node", "local"), None, None),
        P(("node", "local"), None, None),
        P(("node", "local"), None, None),
    )
    return jax.shard_map(
        local,
        mesh=mesh,
        in_specs=placed,
        out_specs=(P(("node", "local"), None), P()),
        check_vma=False,
    )
```

```python
import functools

import jax
import jax.numpy as jnp
from jax import lax
from jax.experimental import pallas as pl
from jax.experimental.pallas import tpu as pltpu
from jax.sharding import PartitionSpec as P

MESH = pl.DeviceIdType.MESH
VMEM_LIMIT = 63 * 1024 * 1024
F32, BF16, I16 = jnp.float32, jnp.bfloat16, jnp.int16
AHEAD = 2
LAG = 5
RING = 3


def chunks_of(width):
    return max(n for n in range(1, 11) if width % (n * 128) == 0)


def tile_of(rows):
    return max(n for n in (256, 128, 64, 32, 16, 8) if rows % n == 0)


def greet(nn, nl, mn, ml):
    barrier = pltpu.get_barrier_semaphore()
    for k in range(1, nn):
        pl.semaphore_signal(barrier, inc=1, device_id={"node": lax.rem(mn + k, nn)}, device_id_type=MESH)
    for k in range(1, nl):
        pl.semaphore_signal(barrier, inc=1, device_id={"local": lax.rem(ml + k, nl)}, device_id_type=MESH)
    pl.semaphore_wait(barrier, nn + nl - 2)


def places(info, first, stride, count, topk):
    lines = info.shape[-1]
    expert = (lax.broadcasted_iota(jnp.int32, (count, lines), 0) * stride + first).astype(F32)
    named = jnp.zeros((count, lines), F32)
    weight = jnp.zeros((count, lines), F32)
    for k in range(topk):
        match = info[k : k + 1, :] == expert
        named = jnp.where(match, 1.0, named)
        weight = jnp.where(match, info[8 + k : 9 + k, :], weight)
    earlier = (
        lax.broadcasted_iota(jnp.int32, (lines, lines), 0) < lax.broadcasted_iota(jnp.int32, (lines, lines), 1)
    ).astype(F32)
    slot = jnp.dot(named, earlier, preferred_element_type=F32)
    return jnp.where(named > 0.0, slot, -1.0), weight


def chooser(info, first, stride, count, topk, cap):
    slot, _ = places(info, first, stride, count, topk)
    rank = lax.broadcasted_iota(jnp.int32, (cap, info.shape[-1]), 0).astype(F32)
    return jnp.concatenate(
        [jnp.where(slot[e : e + 1, :] == rank, 1.0, 0.0) for e in range(count)], axis=0
    ).astype(BF16)


def mixer(info, first, stride, count, topk, cap):
    slot, weight = places(info, first, stride, count, topk)
    rank = lax.broadcasted_iota(jnp.int32, (cap, info.shape[-1]), 0).astype(F32)
    back = jnp.concatenate(
        [jnp.where(slot[e : e + 1, :] == rank, weight[e : e + 1, :], 0.0) for e in range(count)], axis=0
    ).T
    high = back.astype(BF16)
    rest = back - high.astype(F32)
    middle = rest.astype(BF16)
    return jnp.concatenate([high, middle, (rest - middle.astype(F32)).astype(BF16)], axis=0)


def remote(src, dst, send, recv, **place):
    return pltpu.make_async_remote_copy(
        src_ref=src, dst_ref=dst, send_sem=send, recv_sem=recv, device_id=place, device_id_type=MESH
    )


def layer_kernel(
    nn, nl, nch, npl, cap, topk,
    tok, routes, gains, wg, wu, wd,
    out, loss,
    held, flat, sent, arrived, hid, dbuf, infos, peers, tallies, tally,
    got, got_scale, met, got_slim, got_thin,
    up_send, up_recv, dn_send, dn_recv, p_send, p_recv, g_send, g_recv, f_send, f_recv, v_send, v_recv,
    i_send, i_recv, j_send, j_recv, t_send, t_recv, own_sem, w_sem, d_sem,
    o_send, o_recv, z_send, z_recv, s_send, s_recv, V_send, V_recv, x_send, x_recv, q_send, q_recv, r_send, r_recv,
    free, free_up,
):
    mn, ml = lax.axis_index("node"), lax.axis_index("local")
    lines, width = tok.shape
    ch = width // nch
    nz = nch - npl
    ff = wg.shape[1]
    rows = nn * cap
    experts = nn * nl
    chips = max(nl // 2, 1)
    core = lax.rem(ml, 2)
    chip = ml // 2
    sibling = ml + 1 - 2 * core
    step = tile_of(nl * rows)
    wide = step // rows
    near, far = pl.ds(0, cap), pl.ds(cap, rows - cap)

    def cols(c):
        return pl.ds(pl.multiple_of(c * ch, 128), ch)

    def slots_of(e):
        return pl.ds(pl.multiple_of(e * cap, cap), cap)

    def chunk_at(t):
        return jnp.where(t == 0, 0, jnp.where(t <= npl, nz + t - 1, t - npl))

    def down_weights(t):
        slot = lax.rem(t, RING)
        return pltpu.make_async_copy(wd.at[:, cols(chunk_at(t))], dbuf.at[slot], d_sem.at[slot])

    def give(c, at, l, send, recv):
        k = lax.rem(l - ml + nl, nl)
        return remote(sent.at[c, l, at, :], arrived.at[c, ml, at, :], send.at[c, k - 1], recv.at[c, k - 1], local=l)

    def take(c, at, k, send, recv):
        e = lax.rem(ml + nl - k, nl)
        return remote(arrived.at[c, e, at, :], arrived.at[c, e, at, :], send.at[c, k - 1], recv.at[c, k - 1], local=e)

    def first_half(acc, wbuf, pick, choose):
        def weights(c):
            slot = lax.rem(c, RING)
            return (
                pltpu.make_async_copy(wg.at[cols(c), :], wbuf.at[slot, :, pl.ds(0, ff)], w_sem.at[slot, 0]),
                pltpu.make_async_copy(wu.at[cols(c), :], wbuf.at[slot, :, pl.ds(ff, ff)], w_sem.at[slot, 1]),
            )

        def own(c):
            return pltpu.make_async_copy(tok.at[:, cols(c)], held.at[c, mn], own_sem.at[c])

        def up(c, d, block):
            return remote(held.at[c, block], held.at[c, block], up_send.at[c, d], up_recv.at[c, d], node=mn + 1)

        def down(c, d, block):
            return remote(held.at[c, block], held.at[c, block], dn_send.at[c, d], dn_recv.at[c, d], node=mn - 1)

        def within(c, at, k):
            e = lax.rem(ml + k, nl)
            return remote(
                sent.at[c, e, at, :], arrived.at[c, ml, at, :], p_send.at[c, k - 1], p_recv.at[c, k - 1], local=e
            )

        def within_all(c, k):
            at = arrived.at[c, lax.rem(ml + nl - k, nl)]
            return remote(at, at, p_send.at[c, k - 1], p_recv.at[c, k - 1], local=lax.rem(ml + nl - k, nl))

        def own_flat(q):
            return pltpu.make_async_copy(tok.at[:, cols(nz + q)], flat.at[q, ml], own_sem.at[nz + q])

        def abroad(q, j):
            to = lax.rem(chip + j, chips) * 2 + core
            return remote(flat.at[q, ml], flat.at[q, ml], g_send.at[q, j - 1], g_recv.at[q, j - 1], local=to)

        def from_abroad(q, j):
            at = lax.rem(chip + chips - j, chips) * 2 + core
            return remote(flat.at[q, at], flat.at[q, at], g_send.at[q, j - 1], g_recv.at[q, j - 1], local=at)

        def across(q, j):
            at = lax.rem(chip + chips - j, chips) * 2 + core
            return remote(flat.at[q, at], flat.at[q, at], f_send.at[q, j], f_recv.at[q, j], local=sibling)

        def from_across(q, j):
            at = lax.rem(chip + chips - j, chips) * 2 + 1 - core
            return remote(flat.at[q, at], flat.at[q, at], f_send.at[q, j], f_recv.at[q, j], local=sibling)

        def upright(q, k):
            n = lax.rem(mn + k, nn)
            return remote(
                sent.at[nz + q, :, slots_of(n), :], arrived.at[nz + q, :, pl.ds((nn - k) * cap, cap), :],
                v_send.at[q, k - 1], v_recv.at[q, k - 1], node=n,
            )

        def info_copy(k):
            return remote(infos.at[mn], infos.at[mn], i_send.at[k - 1], i_recv.at[k - 1], node=lax.rem(mn + k, nn))

        def peer_copy(k):
            return remote(peers.at[ml], peers.at[ml], j_send.at[k - 1], j_recv.at[k - 1], local=lax.rem(ml + k, nl))

        def tally_copy(k):
            return remote(tally, tallies.at[ml], t_send.at[k - 1], t_recv.at[k - 1], local=lax.rem(ml + k, nl))

        def start_own(c):
            @pl.when(mn + 1 < nn)
            def _():
                up(c, 0, mn).start()

            @pl.when(mn > 0)
            def _():
                down(c, 0, mn).start()

        for q in range(npl):
            own_flat(q).start()

        @pl.loop(0, nz)
        def _(c):
            own(c).start()

        @pl.loop(0, min(RING, nch))
        def _(c):
            for copy in weights(c):
                copy.start()
            down_weights(c).start()

        mine = jnp.concatenate(
            [routes[...].astype(F32), jnp.zeros((8 - topk, lines), F32), gains[...], jnp.zeros((8 - topk, lines), F32)], axis=0
        )
        infos[mn] = mine
        peers[ml] = mine
        pick[mn] = chooser(mine, mn * nl, 1, nl, topk, cap)
        greet(nn, nl, mn, ml)

        for q in range(npl):
            own_flat(q).wait()
            for j in range(1, chips):
                abroad(q, j).start()
            across(q, 0).start()

        @pl.loop(0, AHEAD)
        def _(c):
            own(c).wait()
            start_own(c)

        for k in range(1, nn):
            info_copy(k).start()
        for k in range(1, nl):
            peer_copy(k).start()

        def choose_rows(c, j):
            n = lax.rem(mn + j, nn)
            rows_of = jnp.dot(pick[n], held[c, n], preferred_element_type=F32)
            sent[c, :, slots_of(j), :] = rows_of.reshape(nl, cap, ch).astype(BF16)

        def hand_out(c, at):
            for k in range(1, nl):
                within(c, at, k).start()
            arrived[c, ml, at, :] = sent[c, ml, at, :]

        @pl.loop(0, nz)
        def _(c):
            @pl.when(c >= AHEAD)
            def _():
                own(c).wait()

            choose_rows(c, 0)
            hand_out(c, near)

        for k in range(1, nn):
            info_copy(k).wait_recv()

        @pl.loop(0, nn)
        def _(n):
            @pl.when(n != mn)
            def _():
                pick[n] = chooser(infos[n], mn * nl, 1, nl, topk, cap)

        acc[...] = jnp.zeros(acc.shape, F32)

        def product(c, m):
            block = arrived[c, pl.ds(m * wide, wide)].reshape(step, ch)
            return jnp.dot(block, wbuf[lax.rem(c, RING)], preferred_element_type=F32)

        def multiply(c):
            for copy in weights(c):
                copy.wait()

            @pl.loop(0, nl // wide)
            def _(m):
                acc[pl.ds(pl.multiple_of(m * step, step), step), :] += product(c, m)

            @pl.when(c + RING < nch)
            def _():
                for copy in weights(c + RING):
                    copy.start()

        def hand_up(q):
            for j in range(chips):
                from_across(q, j).wait_recv()

            @pl.loop(0, nl)
            def _(l):
                sent[nz + q, l] = jnp.dot(choose[l], flat[q, l], preferred_element_type=F32).astype(BF16)
                arrived[nz + q, l, near, :] = sent[nz + q, l, slots_of(mn), :]

            for k in range(1, nn):
                upright(q, k).start()

        first_up = min(3, nz - 1)

        @pl.loop(0, nz + LAG)
        def _(i):
            @pl.when(i < nz)
            def _():
                @pl.when(i + AHEAD < nz)
                def _():
                    start_own(i + AHEAD)

                for d in range(nn - 1):
                    @pl.when(mn - 1 - d >= 0)
                    def _():
                        block = mn - 1 - d
                        up(i, d, block).wait_recv()

                        if d + 1 < nn - 1:
                            @pl.when(mn + 1 < nn)
                            def _():
                                up(i, d + 1, block).start()

                    @pl.when(mn + 1 + d < nn)
                    def _():
                        block = mn + 1 + d
                        down(i, d, block).wait_recv()

                        if d + 1 < nn - 1:
                            @pl.when(mn > 0)
                            def _():
                                down(i, d + 1, block).start()

                @pl.loop(1, nn)
                def _(j):
                    choose_rows(i, j)

                hand_out(i, far)

            if npl:
                @pl.when(i == 0)
                def _():
                    for k in range(1, nl):
                        peer_copy(k).wait_recv()

                    @pl.loop(0, nl)
                    def _(l):
                        choose[l] = chooser(peers[l], ml, nl, nn, topk, cap)

                @pl.when(i == min(1, nz - 1))
                def _():
                    for q in range(npl):
                        for j in range(1, chips):
                            from_abroad(q, j).wait_recv()
                            across(q, j).start()

                for q in range(npl):
                    @pl.when(i == (nz - 1 if q == npl - 1 else first_up + q))
                    def _():
                        hand_up(q)

            @pl.when((i >= LAG) & (i - LAG < nch - 1))
            def _():
                for k in range(1, nl):
                    within_all(i - LAG, k).wait_recv()
                multiply(i - LAG)

            @pl.when(i == 0)
            def _():
                label = lax.broadcasted_iota(jnp.int32, (tally.shape[1], lines), 0).astype(F32)
                hits = jnp.zeros(label.shape, F32)
                sums = jnp.zeros(label.shape, F32)
                for n in range(nn):
                    for k in range(topk):
                        match = infos[n, k : k + 1, :] == label
                        hits = hits + jnp.where(match, 1.0, 0.0)
                        sums = sums + jnp.where(match, infos[n, 8 + k : 9 + k, :], 0.0)
                line = lax.broadcasted_iota(jnp.int32, (8, tally.shape[1]), 0)
                both = jnp.where(
                    line == 0,
                    jnp.sum(hits.T, axis=0, keepdims=True),
                    jnp.where(line == 1, jnp.sum(sums.T, axis=0, keepdims=True), 0.0),
                )
                tally[...] = both
                tallies[ml] = both
                for k in range(1, nl):
                    tally_copy(k).start()

            @pl.when(i == nz - 1)
            def _():
                for k in range(1, nl):
                    tally_copy(k).wait_recv()
                total = tallies[0]
                for l in range(1, nl):
                    total = total + tallies[l]
                tokens = float(lines * experts)
                loss[...] = jnp.sum(total[0:1, :] * total[1:2, :], axis=1, keepdims=True) * (
                    experts / (topk * tokens * tokens)
                )

        last = nch - 1
        for k in range(1, nl):
            pl.semaphore_signal(free, inc=1, device_id={"local": lax.rem(ml + k, nl)}, device_id_type=MESH)

        if npl:
            @pl.loop(0, npl - 1)
            def _(q):
                for k in range(1, nn):
                    upright(q, k).wait_recv()
                multiply(nz + q)

            for k in range(1, nn):
                upright(npl - 1, k).wait_recv()
        else:
            for k in range(1, nl):
                within_all(last, k).wait_recv()
        for copy in weights(last):
            copy.wait()
        for k in range(1, nl):
            within_all(0, k).wait_send()
        down_weights(0).wait()
        pl.semaphore_wait(free, nl - 1)

        @pl.loop(0, nl // wide)
        def _(i):
            m = lax.rem(ml // wide + 1 + i, nl // wide)
            at = pl.ds(pl.multiple_of(m * step, step), step)
            both = acc[at, :] + product(last, m)
            gate = both[:, 0:ff]
            short = (gate / (1.0 + jnp.exp(-gate)) * both[:, ff : 2 * ff]).astype(BF16)
            hid[at, :] = short
            value = jnp.dot(short, dbuf[0], preferred_element_type=F32)
            sent[0, pl.ds(m * wide, wide)] = value.astype(BF16).reshape(wide, rows, ch)
            for u in range(wide):
                l = m * wide + u

                @pl.when(l != ml)
                def _():
                    give(0, far, l, p_send, p_recv).start()

                @pl.when(l == ml)
                def _():
                    arrived[0, ml] = sent[0, ml]

        for k in range(1, nn if npl else nl):
            to = {"node": lax.rem(mn + k, nn)} if npl else {"local": lax.rem(ml + k, nl)}
            pl.semaphore_signal(free_up, inc=1, device_id=to, device_id_type=MESH)

        @pl.when(RING < nch)
        def _():
            down_weights(RING).start()

        for k in range(1, nn):
            info_copy(k).wait_send()
        for k in range(1, nl):
            tally_copy(k).wait_send()
            peer_copy(k).wait_send()
            if not npl:
                peer_copy(k).wait_recv()
        for q in range(npl):
            across(q, 0).wait_send()
            for j in range(1, chips):
                abroad(q, j).wait_send()
                across(q, j).wait_send()
            for k in range(1, nn):
                upright(q, k).wait_send()

        @pl.loop(0, nz)
        def _(c):
            @pl.when(c > 0)
            def _():
                for k in range(1, nl):
                    within_all(c, k).wait_send()

            for d in range(nn - 1):
                @pl.when((mn + 1 < nn) & (mn - d >= 0))
                def _():
                    up(c, d, mn - d).wait_send()

                @pl.when((mn > 0) & (mn + d < nn))
                def _():
                    down(c, d, mn + d).wait_send()


    def second_half(mix, blur, work, part, scale, kept, lent, slim, thin):
        def along(c, p, toward):
            mine = jnp.where(p < mn, p, p - 1)
            there = jnp.where(p > mn, p, jnp.where(p == mn - 1, nn, p))
            return (
                remote(part.at[c, mine], got.at[c, there], z_send.at[c, mine], z_recv.at[c, there], node=mn + toward),
                remote(scale.at[c, mine], got_scale.at[c, there], s_send.at[c, mine], s_recv.at[c, there], node=mn + toward),
            )

        def land(c, slot, toward):
            for buffer, sem in ((got, z_recv), (got_scale, s_recv)):
                at = buffer.at[c, slot]
                remote(at, at, sem.at[c, slot], sem.at[c, slot], node=mn - toward).wait_recv()

        def ascend(q, k):
            n = lax.rem(mn + k, nn)
            return remote(
                sent.at[nz + q, :, pl.ds(k * cap, cap), :], arrived.at[nz + q, :, slots_of(mn), :], V_send.at[q, k - 1], V_recv.at[q, k - 1], node=n
            )

        def lend(q, j):
            return remote(lent.at[q, j], met.at[q, j], x_send.at[q, j], x_recv.at[q, j], local=sibling)

        def deal(q, j):
            to = lax.rem(chip + j, chips) * 2 + core
            return (
                remote(slim.at[q, j - 1], got_slim.at[q, j - 1], q_send.at[q, j - 1], q_recv.at[q, j - 1], local=to),
                remote(thin.at[q, j - 1], got_thin.at[q, j - 1], r_send.at[q, j - 1], r_recv.at[q, j - 1], local=to),
            )

        pl.semaphore_wait(free_up, (nn if npl else nl) - 1)

        @pl.loop(1, nch)
        def _(t):
            c = chunk_at(t)
            slot = lax.rem(t, RING)
            down_weights(t).wait()

            @pl.loop(0, nl // wide)
            def _(m):
                at = pl.ds(pl.multiple_of(m * step, step), step)
                value = jnp.dot(hid[at, :], dbuf[slot], preferred_element_type=F32)
                sent[c, pl.ds(m * wide, wide)] = value.astype(BF16).reshape(wide, rows, ch)

            @pl.when(t + RING < nch)
            def _():
                down_weights(t + RING).start()

            if npl:
                @pl.when(t <= npl)
                def _():
                    for k in range(1, nn):
                        ascend(t - 1, k).start()

                    @pl.loop(0, nl)
                    def _(l):
                        arrived[c, l, slots_of(mn), :] = sent[c, l, near, :]

            @pl.when(t > npl)
            def _():
                for k in range(1, nl):
                    give(c, far, lax.rem(ml + k, nl), p_send, p_recv).start()
                arrived[c, ml] = sent[c, ml]

        @pl.loop(0, nn)
        def _(n):
            mix[n] = mixer(infos[n], mn * nl, 1, nl, topk, cap)

        if npl:
            @pl.loop(0, nl)
            def _(l):
                blur[l] = mixer(peers[l], ml, nl, nn, topk, cap)

        diagonal = lax.broadcasted_iota(jnp.int32, (lines, lines), 0) == lax.broadcasted_iota(jnp.int32, (lines, lines), 1)

        def summed(terms):
            return terms[0:lines] + terms[lines : 2 * lines] + terms[2 * lines : 3 * lines]

        def blend(c, n):
            block = arrived[c, :, slots_of(lax.rem(n - mn + nn, nn)), :].reshape(nl * cap, ch)
            return summed(jnp.dot(mix[n], block, preferred_element_type=F32))

        def pack(value):
            peak = jnp.maximum(jnp.max(jnp.abs(value), axis=1, keepdims=True), 1e-30)
            short = jnp.round(value * (32767.0 / peak)).astype(jnp.int32).astype(I16)
            line = jnp.sum(jnp.where(diagonal, peak, 0.0), axis=0, keepdims=True)
            return short, jnp.broadcast_to(line, (8, lines))

        def unpack(short, line):
            peak = jnp.sum(jnp.where(diagonal, line[0:1, :], 0.0), axis=1, keepdims=True)
            return short.astype(jnp.int32).astype(F32) * (peak * (1.0 / 32767.0))

        def pass_on(c, p, toward, relay):
            work[...] = blend(c, p)

            @pl.when(relay)
            def _():
                land(c, p, toward)
                work[...] += unpack(got[c, p], got_scale[c, p])

            mine = jnp.where(p < mn, p, p - 1)
            part[c, mine], scale[c, mine] = pack(work[...])
            for copy in along(c, p, toward):
                copy.start()

        late = max(nz - 2, 0)

        @pl.loop(0, nz + nn - 2)
        def _(i):
            @pl.when(i < nz)
            def _():
                for k in range(1, nl):
                    take(i, far, k, p_send, p_recv).wait_recv()

            c_up = i - mn
            c_down = i - (nn - 1 - mn)
            for d in reversed(range(nn - 1)):
                @pl.when((c_up >= 0) & (c_up < nz) & (mn + 1 + d < nn))
                def _():
                    pass_on(c_up, mn + 1 + d, 1, mn > 0)

                @pl.when((c_down >= 0) & (c_down < nz) & (mn - 1 - d >= 0))
                def _():
                    pass_on(c_down, mn - 1 - d, -1, mn < nn - 1)

            @pl.when(i == late)
            def _():
                @pl.loop(0, nz)
                def _(c):
                    for k in range(1, nl):
                        give(c, near, lax.rem(ml + k, nl), o_send, o_recv).start()

            if npl:
                @pl.when(i == late)
                def _():
                    for q in range(npl):
                        for k in range(1, nn):
                            ascend(q, k).wait_recv()

                        @pl.loop(0, chips)
                        def _(j):
                            to = lax.rem(chip + j, chips) * 2
                            lent[q, j] = summed(
                                jnp.dot(blur[to + 1 - core], arrived[nz + q, to + 1 - core], preferred_element_type=F32)
                            )
                            lend(q, j).start()
                            kept[q, j] = summed(jnp.dot(blur[to + core], arrived[nz + q, to + core], preferred_element_type=F32))

                @pl.when(i == late + 1)
                def _():
                    for q in range(npl):
                        for j in range(chips):
                            lend(q, j).wait_recv()
                            if j:
                                slim[q, j - 1], thin[q, j - 1] = pack(kept[q, j] + met[q, j])
                                for copy in deal(q, j):
                                    copy.start()

        @pl.loop(0, nz)
        def _(c):
            for k in range(1, nl):
                take(c, near, k, o_send, o_recv).wait_recv()
            work[...] = blend(c, mn)

            @pl.when(mn > 0)
            def _():
                land(c, mn, 1)
                work[...] += unpack(got[c, mn], got_scale[c, mn])

            @pl.when(mn < nn - 1)
            def _():
                land(c, nn, -1)
                work[...] += unpack(got[c, nn], got_scale[c, nn])

            out[:, cols(c)] = work[...].astype(out.dtype)

        for q in range(npl):
            total = kept[q, 0] + met[q, 0]
            for j in range(1, chips):
                for copy in deal(q, j):
                    copy.wait_recv()
                total = total + unpack(got_slim[q, j - 1], got_thin[q, j - 1])
            out[:, cols(nz + q)] = total.astype(out.dtype)

        for q in range(npl):
            for k in range(1, nn):
                ascend(q, k).wait_send()
            for j in range(chips):
                lend(q, j).wait_send()
                if j:
                    for copy in deal(q, j):
                        copy.wait_send()

        @pl.loop(0, nz)
        def _(c):
            for k in range(1, nl):
                give(c, far, lax.rem(ml + k, nl), p_send, p_recv).wait_send()
                give(c, near, lax.rem(ml + k, nl), o_send, o_recv).wait_send()
            for d in range(nn - 1):
                @pl.when(mn + 1 + d < nn)
                def _():
                    for copy in along(c, mn + 1 + d, 1):
                        copy.wait_send()

                @pl.when(mn - 1 - d >= 0)
                def _():
                    for copy in along(c, mn - 1 - d, -1):
                        copy.wait_send()


    some, others = max(npl, 1), max(chips - 1, 1)
    pl.run_scoped(
        first_half,
        pltpu.VMEM((nl * rows, 2 * ff), F32),
        pltpu.VMEM((RING, ch, 2 * ff), BF16),
        pltpu.VMEM((nn, nl * cap, lines), BF16),
        pltpu.VMEM((nl, rows, lines), BF16),
    )
    pl.run_scoped(
        second_half,
        pltpu.VMEM((nn, 3 * lines, nl * cap), BF16),
        pltpu.VMEM((nl, 3 * lines, rows), BF16),
        pltpu.VMEM((lines, ch), F32),
        pltpu.VMEM((nz, nn - 1, lines, ch), I16),
        pltpu.VMEM((nz, nn - 1, 8, lines), F32),
        pltpu.VMEM((some, chips, lines, ch), F32),
        pltpu.VMEM((some, chips, lines, ch), F32),
        pltpu.VMEM((some, others, lines, ch), I16),
        pltpu.VMEM((some, others, 8, lines), F32),
    )


def sems(*shape):
    return pltpu.SemaphoreType.DMA(tuple(max(n, 1) for n in shape))


def local(tokens, routes, route_weights, w_gate, w_up, w_down):
    nn, nl = lax.axis_size("node"), lax.axis_size("local")
    exp_dev, width, ff = w_gate.shape
    experts = exp_dev * nn * nl
    assert exp_dev == 1
    lines, topk = routes.shape
    assert topk <= 8
    cap = 4 * lines * topk // (3 * experts)
    rows = nn * cap
    nch = chunks_of(width)
    ch = width // nch
    held_bytes = 2 * lines * width * 3 * nn + 4 * nl * rows * width
    npl = nch // 10 if nl % 2 == 0 and held_bytes <= VMEM_LIMIT * 3 // 4 else 0
    nz = nch - npl
    some = max(npl, 1)
    chips = max(nl // 2, 1)
    others = max(chips - 1, 1)
    spare = 1 if npl == 0 else nl
    wide = -(-experts // 128) * 128

    vmem = pl.BlockSpec(memory_space=pltpu.VMEM)
    hbm = pl.BlockSpec(memory_space=pl.ANY)
    mixed, loss = pl.pallas_call(
        functools.partial(layer_kernel, nn, nl, nch, npl, cap, topk),
        out_shape=(jax.ShapeDtypeStruct((lines, width), tokens.dtype), jax.ShapeDtypeStruct((1, 1), F32)),
        in_specs=[hbm, vmem, vmem, hbm, hbm, hbm],
        out_specs=(vmem, vmem),
        scratch_shapes=[
            pltpu.VMEM((nz, nn, lines, ch), BF16),
            pltpu.VMEM((some, spare, lines, ch), BF16),
            pltpu.VMEM((nch, nl, rows, ch), BF16),
            pltpu.VMEM((nch, nl, rows, ch), BF16),
            pltpu.VMEM((nl * rows, ff), BF16),
            pltpu.VMEM((RING, ff, ch), BF16),
            pltpu.VMEM((nn, 16, lines), F32),
            pltpu.VMEM((nl, 16, lines), F32),
            pltpu.VMEM((nl, 8, wide), F32),
            pltpu.VMEM((8, wide), F32),
            pltpu.VMEM((nz, nn + 1, lines, ch), I16),
            pltpu.VMEM((nz, nn + 1, 8, lines), F32),
            pltpu.VMEM((some, chips if npl else 1, lines, ch), F32),
            pltpu.VMEM((some, others if npl else 1, lines, ch), I16),
            pltpu.VMEM((some, others, 8, lines), F32),
            sems(nz, nn - 1), sems(nz, nn - 1), sems(nz, nn - 1), sems(nz, nn - 1),
            sems(nz, nl - 1), sems(nz, nl - 1),
            sems(some, chips - 1), sems(some, chips - 1), sems(some, chips), sems(some, chips),
            sems(some, nn - 1), sems(some, nn - 1),
            sems(nn - 1), sems(nn - 1), sems(nl - 1), sems(nl - 1), sems(nl - 1), sems(nl - 1),
            sems(nch), sems(RING, 2), sems(RING),
            sems(nz, nl - 1), sems(nz, nl - 1),
            sems(nz, nn - 1), sems(nz, nn + 1), sems(nz, nn - 1), sems(nz, nn + 1),
            sems(some, nn - 1), sems(some, nn - 1), sems(some, chips), sems(some, chips),
            sems(some, chips - 1), sems(some, chips - 1), sems(some, chips - 1), sems(some, chips - 1),
            pltpu.SemaphoreType.REGULAR, pltpu.SemaphoreType.REGULAR,
        ],
        compiler_params=pltpu.CompilerParams(collective_id=0, has_side_effects=True, vmem_limit_bytes=VMEM_LIMIT),
    )(tokens, routes.T, route_weights.T, w_gate[0], w_up[0], w_down[0])
    return (mixed, loss.reshape(()))


def solution(mesh):
    placed = (
        P(("node", "local"), None),
        P(("node", "local"), None),
        P(("node", "local"), None),
        P(("node", "local"), None, None),
        P(("node", "local"), None, None),
        P(("node", "local"), None, None),
    )
    return jax.shard_map(
        local,
        mesh=mesh,
        in_specs=placed,
        out_specs=(P(("node", "local"), None), P()),
        check_vma=False,
    )
```

```python
import functools

import jax
import jax.numpy as jnp
from jax import lax
from jax.experimental import pallas as pl
from jax.experimental.pallas import tpu as pltpu
from jax.sharding import PartitionSpec as P

MESH = pl.DeviceIdType.MESH
VMEM_LIMIT = 63 * 1024 * 1024
F32, BF16, I16 = jnp.float32, jnp.bfloat16, jnp.int16
AHEAD = 2
LAG = 5
RING = 3


def chunks_of(width):
    return max(n for n in range(1, 11) if width % (n * 128) == 0)


def tile_of(rows):
    return max(n for n in (256, 128, 64, 32, 16, 8) if rows % n == 0)


def greet(nn, nl, mn, ml):
    barrier = pltpu.get_barrier_semaphore()
    for k in range(1, nn):
        pl.semaphore_signal(barrier, inc=1, device_id={"node": lax.rem(mn + k, nn)}, device_id_type=MESH)
    for k in range(1, nl):
        pl.semaphore_signal(barrier, inc=1, device_id={"local": lax.rem(ml + k, nl)}, device_id_type=MESH)


def places(info, first, stride, count, topk):
    lines = info.shape[-1]
    expert = (lax.broadcasted_iota(jnp.int32, (count, lines), 0) * stride + first).astype(F32)
    named = jnp.zeros((count, lines), F32)
    weight = jnp.zeros((count, lines), F32)
    for k in range(topk):
        match = info[k : k + 1, :] == expert
        named = jnp.where(match, 1.0, named)
        weight = jnp.where(match, info[8 + k : 9 + k, :], weight)
    earlier = (
        lax.broadcasted_iota(jnp.int32, (lines, lines), 0) < lax.broadcasted_iota(jnp.int32, (lines, lines), 1)
    ).astype(F32)
    slot = jnp.dot(named, earlier, preferred_element_type=F32)
    return jnp.where(named > 0.0, slot, -1.0), weight


def chooser(info, first, stride, count, topk, cap):
    slot, _ = places(info, first, stride, count, topk)
    rank = lax.broadcasted_iota(jnp.int32, (cap, info.shape[-1]), 0).astype(F32)
    return jnp.concatenate(
        [jnp.where(slot[e : e + 1, :] == rank, 1.0, 0.0) for e in range(count)], axis=0
    ).astype(BF16)


def mixer(info, first, stride, count, topk, cap):
    slot, weight = places(info, first, stride, count, topk)
    rank = lax.broadcasted_iota(jnp.int32, (cap, info.shape[-1]), 0).astype(F32)
    back = jnp.concatenate(
        [jnp.where(slot[e : e + 1, :] == rank, weight[e : e + 1, :], 0.0) for e in range(count)], axis=0
    ).T
    high = back.astype(BF16)
    rest = back - high.astype(F32)
    middle = rest.astype(BF16)
    return jnp.concatenate([high, middle, (rest - middle.astype(F32)).astype(BF16)], axis=0)


def remote(src, dst, send, recv, **place):
    return pltpu.make_async_remote_copy(
        src_ref=src, dst_ref=dst, send_sem=send, recv_sem=recv, device_id=place, device_id_type=MESH
    )


def layer_kernel(
    nn, nl, nch, npl, cap, topk,
    tok, routes, gains, wg, wu, wd,
    out, loss,
    held, flat, sent, arrived, hid, dbuf, infos, peers, tallies, tally,
    got, got_scale, met, got_slim, got_thin,
    up_send, up_recv, dn_send, dn_recv, p_send, p_recv, g_send, g_recv, f_send, f_recv, v_send, v_recv,
    i_send, i_recv, j_send, j_recv, t_send, t_recv, own_sem, w_sem, d_sem,
    o_send, o_recv, z_send, z_recv, s_send, s_recv, V_send, V_recv, x_send, x_recv, q_send, q_recv, r_send, r_recv,
    free, free_up, free_last,
):
    mn, ml = lax.axis_index("node"), lax.axis_index("local")
    lines, width = tok.shape
    ch = width // nch
    nz = nch - npl
    ff = wg.shape[1]
    rows = nn * cap
    experts = nn * nl
    chips = max(nl // 2, 1)
    core = lax.rem(ml, 2)
    chip = ml // 2
    sibling = ml + 1 - 2 * core
    step = tile_of(nl * rows)
    wide = step // rows
    near, far = pl.ds(0, cap), pl.ds(cap, rows - cap)

    def cols(c):
        return pl.ds(pl.multiple_of(c * ch, 128), ch)

    def slots_of(e):
        return pl.ds(pl.multiple_of(e * cap, cap), cap)

    def chunk_at(t):
        return jnp.where(t == 0, 0, jnp.where(t <= npl, nz + t - 1, t - npl))

    def down_weights(t):
        slot = lax.rem(t, RING)
        return pltpu.make_async_copy(wd.at[:, cols(chunk_at(t))], dbuf.at[slot], d_sem.at[slot])

    def give(c, at, l, send, recv):
        k = lax.rem(l - ml + nl, nl)
        return remote(sent.at[c, l, at, :], arrived.at[c, ml, at, :], send.at[c, k - 1], recv.at[c, k - 1], local=l)

    def take(c, at, k, send, recv):
        e = lax.rem(ml + nl - k, nl)
        return remote(arrived.at[c, e, at, :], arrived.at[c, e, at, :], send.at[c, k - 1], recv.at[c, k - 1], local=e)

    def first_half(acc, wbuf, pick, choose):
        def chunk_of(u):
            return jnp.where(u < nz - 1, u, jnp.where(u < nch - 1, u + 1, nz - 1))

        def weights(u):
            slot, c = lax.rem(u, RING), chunk_of(u)
            return (
                pltpu.make_async_copy(wg.at[cols(c), :], wbuf.at[slot, :, pl.ds(0, ff)], w_sem.at[slot, 0]),
                pltpu.make_async_copy(wu.at[cols(c), :], wbuf.at[slot, :, pl.ds(ff, ff)], w_sem.at[slot, 1]),
            )

        def own(c):
            return pltpu.make_async_copy(tok.at[:, cols(c)], held.at[c, mn], own_sem.at[c])

        def up(c, d, block):
            return remote(held.at[c, block], held.at[c, block], up_send.at[c, d], up_recv.at[c, d], node=mn + 1)

        def down(c, d, block):
            return remote(held.at[c, block], held.at[c, block], dn_send.at[c, d], dn_recv.at[c, d], node=mn - 1)

        def within(c, at, k):
            e = lax.rem(ml + k, nl)
            return remote(
                sent.at[c, e, at, :], arrived.at[c, ml, at, :], p_send.at[c, k - 1], p_recv.at[c, k - 1], local=e
            )

        def within_all(c, k):
            at = arrived.at[c, lax.rem(ml + nl - k, nl)]
            return remote(at, at, p_send.at[c, k - 1], p_recv.at[c, k - 1], local=lax.rem(ml + nl - k, nl))

        def own_flat(q):
            return pltpu.make_async_copy(tok.at[:, cols(nz + q)], flat.at[q, ml], own_sem.at[nz + q])

        def abroad(q, j):
            to = lax.rem(chip + j, chips) * 2 + core
            return remote(flat.at[q, ml], flat.at[q, ml], g_send.at[q, j - 1], g_recv.at[q, j - 1], local=to)

        def from_abroad(q, j):
            at = lax.rem(chip + chips - j, chips) * 2 + core
            return remote(flat.at[q, at], flat.at[q, at], g_send.at[q, j - 1], g_recv.at[q, j - 1], local=at)

        def across(q, j):
            at = lax.rem(chip + chips - j, chips) * 2 + core
            return remote(flat.at[q, at], flat.at[q, at], f_send.at[q, j], f_recv.at[q, j], local=sibling)

        def from_across(q, j):
            at = lax.rem(chip + chips - j, chips) * 2 + 1 - core
            return remote(flat.at[q, at], flat.at[q, at], f_send.at[q, j], f_recv.at[q, j], local=sibling)

        def upright(q, k):
            n = lax.rem(mn + k, nn)
            return remote(
                sent.at[nz + q, :, slots_of(n), :], arrived.at[nz + q, :, pl.ds((nn - k) * cap, cap), :],
                v_send.at[q, k - 1], v_recv.at[q, k - 1], node=n,
            )

        def info_copy(k):
            return remote(infos.at[mn], infos.at[mn], i_send.at[k - 1], i_recv.at[k - 1], node=lax.rem(mn + k, nn))

        def peer_copy(k):
            return remote(peers.at[ml], peers.at[ml], j_send.at[k - 1], j_recv.at[k - 1], local=lax.rem(ml + k, nl))

        def tally_copy(k):
            return remote(tally, tallies.at[ml], t_send.at[k - 1], t_recv.at[k - 1], local=lax.rem(ml + k, nl))

        def start_own(c):
            @pl.when(mn + 1 < nn)
            def _():
                up(c, 0, mn).start()

            @pl.when(mn > 0)
            def _():
                down(c, 0, mn).start()

        greet(nn, nl, mn, ml)
        for q in range(npl):
            own_flat(q).start()

        @pl.loop(0, nz)
        def _(c):
            own(c).start()

        @pl.loop(0, min(RING, nch))
        def _(c):
            for copy in weights(c):
                copy.start()
            down_weights(c).start()

        mine = jnp.concatenate(
            [routes[...].astype(F32), jnp.zeros((8 - topk, lines), F32), gains[...], jnp.zeros((8 - topk, lines), F32)], axis=0
        )
        infos[mn] = mine
        peers[ml] = mine
        pl.semaphore_wait(pltpu.get_barrier_semaphore(), nn + nl - 2)

        for q in range(npl):
            own_flat(q).wait()
            for j in range(1, chips):
                abroad(q, j).start()
            across(q, 0).start()

        @pl.loop(0, AHEAD)
        def _(c):
            own(c).wait()
            start_own(c)

        for k in range(1, nn):
            info_copy(k).start()
        for k in range(1, nl):
            peer_copy(k).start()
        pick[mn] = chooser(mine, mn * nl, 1, nl, topk, cap)

        def choose_rows(c, j):
            n = lax.rem(mn + j, nn)
            rows_of = jnp.dot(pick[n], held[c, n], preferred_element_type=F32)
            sent[c, :, slots_of(j), :] = rows_of.reshape(nl, cap, ch).astype(BF16)

        def hand_out(c, at):
            for k in range(1, nl):
                within(c, at, k).start()
            arrived[c, ml, at, :] = sent[c, ml, at, :]

        @pl.loop(0, nz)
        def _(c):
            @pl.when(c >= AHEAD)
            def _():
                own(c).wait()

            choose_rows(c, 0)
            hand_out(c, near)

        for k in range(1, nn):
            info_copy(k).wait_recv()

        @pl.loop(0, nn)
        def _(n):
            @pl.when(n != mn)
            def _():
                pick[n] = chooser(infos[n], mn * nl, 1, nl, topk, cap)

        acc[...] = jnp.zeros(acc.shape, F32)

        def product(u, m):
            block = arrived[chunk_of(u), pl.ds(m * wide, wide)].reshape(step, ch)
            return jnp.dot(block, wbuf[lax.rem(u, RING)], preferred_element_type=F32)

        def multiply(u):
            for copy in weights(u):
                copy.wait()

            @pl.loop(0, nl // wide)
            def _(m):
                acc[pl.ds(pl.multiple_of(m * step, step), step), :] += product(u, m)

            @pl.when(u + RING < nch)
            def _():
                for copy in weights(u + RING):
                    copy.start()

        def hand_up(q):
            for j in range(chips):
                from_across(q, j).wait_recv()

            @pl.loop(0, nl)
            def _(l):
                sent[nz + q, l] = jnp.dot(choose[l], flat[q, l], preferred_element_type=F32).astype(BF16)
                arrived[nz + q, l, near, :] = sent[nz + q, l, slots_of(mn), :]

            for k in range(1, nn):
                upright(q, k).start()

        first_up = min(3, nz - 1)

        @pl.loop(0, nz + LAG)
        def _(i):
            @pl.when(i < nz)
            def _():
                @pl.when(i + AHEAD < nz)
                def _():
                    start_own(i + AHEAD)

                for d in range(nn - 1):
                    @pl.when(mn - 1 - d >= 0)
                    def _():
                        block = mn - 1 - d
                        up(i, d, block).wait_recv()

                        if d + 1 < nn - 1:
                            @pl.when(mn + 1 < nn)
                            def _():
                                up(i, d + 1, block).start()

                    @pl.when(mn + 1 + d < nn)
                    def _():
                        block = mn + 1 + d
                        down(i, d, block).wait_recv()

                        if d + 1 < nn - 1:
                            @pl.when(mn > 0)
                            def _():
                                down(i, d + 1, block).start()

                @pl.loop(1, nn)
                def _(j):
                    choose_rows(i, j)

                hand_out(i, far)

            if npl:
                @pl.when(i == 0)
                def _():
                    for k in range(1, nl):
                        peer_copy(k).wait_recv()

                    @pl.loop(0, nl)
                    def _(l):
                        choose[l] = chooser(peers[l], ml, nl, nn, topk, cap)

                @pl.when(i == min(1, nz - 1))
                def _():
                    for q in range(npl):
                        for j in range(1, chips):
                            from_abroad(q, j).wait_recv()
                            across(q, j).start()

                for q in range(npl):
                    @pl.when(i == (nz - 1 if q == npl - 1 else first_up + q))
                    def _():
                        hand_up(q)

            @pl.when((i >= LAG) & (i - LAG < nz - 1))
            def _():
                for k in range(1, nl):
                    within_all(i - LAG, k).wait_recv()
                multiply(i - LAG)

            @pl.when(i == 0)
            def _():
                label = lax.broadcasted_iota(jnp.int32, (tally.shape[1], lines), 0).astype(F32)
                hits = jnp.zeros(label.shape, F32)
                sums = jnp.zeros(label.shape, F32)
                for n in range(nn):
                    for k in range(topk):
                        match = infos[n, k : k + 1, :] == label
                        hits = hits + jnp.where(match, 1.0, 0.0)
                        sums = sums + jnp.where(match, infos[n, 8 + k : 9 + k, :], 0.0)
                line = lax.broadcasted_iota(jnp.int32, (8, tally.shape[1]), 0)
                both = jnp.where(
                    line == 0,
                    jnp.sum(hits.T, axis=0, keepdims=True),
                    jnp.where(line == 1, jnp.sum(sums.T, axis=0, keepdims=True), 0.0),
                )
                tally[...] = both
                tallies[ml] = both
                for k in range(1, nl):
                    tally_copy(k).start()

            @pl.when(i == nz - 1)
            def _():
                for k in range(1, nl):
                    tally_copy(k).wait_recv()
                total = tallies[0]
                for l in range(1, nl):
                    total = total + tallies[l]
                tokens = float(lines * experts)
                loss[...] = jnp.sum(total[0:1, :] * total[1:2, :], axis=1, keepdims=True) * (
                    experts / (topk * tokens * tokens)
                )

        if npl:
            @pl.loop(0, npl)
            def _(q):
                for k in range(1, nn):
                    upright(q, k).wait_recv()
                multiply(nz - 1 + q)

        last = nch - 1
        for k in range(1, nl):
            pl.semaphore_signal(free, inc=1, device_id={"local": lax.rem(ml + k, nl)}, device_id_type=MESH)
        if npl:
            for k in range(1, nn):
                pl.semaphore_signal(free_up, inc=1, device_id={"node": lax.rem(mn + k, nn)}, device_id_type=MESH)
        for copy in weights(last):
            copy.wait()
        for k in range(1, nl):
            within_all(0, k).wait_send()
        down_weights(0).wait()
        pl.semaphore_wait(free, nl - 1)
        for k in range(1, nl):
            within_all(nz - 1, k).wait_recv()

        @pl.loop(0, nl // wide)
        def _(i):
            m = lax.rem(ml // wide + 1 + i, nl // wide)
            at = pl.ds(pl.multiple_of(m * step, step), step)
            both = acc[at, :] + product(last, m)
            gate = both[:, 0:ff]
            short = (gate / (1.0 + jnp.exp(-gate)) * both[:, ff : 2 * ff]).astype(BF16)
            hid[at, :] = short
            value = jnp.dot(short, dbuf[0], preferred_element_type=F32)
            sent[0, pl.ds(m * wide, wide)] = value.astype(BF16).reshape(wide, rows, ch)
            for u in range(wide):
                l = m * wide + u

                @pl.when(l != ml)
                def _():
                    give(0, far, l, p_send, p_recv).start()

                @pl.when(l == ml)
                def _():
                    arrived[0, ml] = sent[0, ml]

        for k in range(1, nl):
            pl.semaphore_signal(free_last, inc=1, device_id={"local": lax.rem(ml + k, nl)}, device_id_type=MESH)

        @pl.when(RING < nch)
        def _():
            down_weights(RING).start()

        for k in range(1, nn):
            info_copy(k).wait_send()
        for k in range(1, nl):
            tally_copy(k).wait_send()
            peer_copy(k).wait_send()
            if not npl:
                peer_copy(k).wait_recv()
        for q in range(npl):
            across(q, 0).wait_send()
            for j in range(1, chips):
                abroad(q, j).wait_send()
                across(q, j).wait_send()
            for k in range(1, nn):
                upright(q, k).wait_send()

        @pl.loop(0, nz)
        def _(c):
            @pl.when(c > 0)
            def _():
                for k in range(1, nl):
                    within_all(c, k).wait_send()

            for d in range(nn - 1):
                @pl.when((mn + 1 < nn) & (mn - d >= 0))
                def _():
                    up(c, d, mn - d).wait_send()

                @pl.when((mn > 0) & (mn + d < nn))
                def _():
                    down(c, d, mn + d).wait_send()


    def second_half(mix, blur, work, part, scale, kept, lent, slim, thin):
        def along(c, p, toward):
            mine = jnp.where(p < mn, p, p - 1)
            there = jnp.where(p > mn, p, jnp.where(p == mn - 1, nn, p))
            return (
                remote(part.at[c, mine], got.at[c, there], z_send.at[c, mine], z_recv.at[c, there], node=mn + toward),
                remote(scale.at[c, mine], got_scale.at[c, there], s_send.at[c, mine], s_recv.at[c, there], node=mn + toward),
            )

        def land(c, slot, toward):
            for buffer, sem in ((got, z_recv), (got_scale, s_recv)):
                at = buffer.at[c, slot]
                remote(at, at, sem.at[c, slot], sem.at[c, slot], node=mn - toward).wait_recv()

        def ascend(q, k):
            n = lax.rem(mn + k, nn)
            return remote(
                sent.at[nz + q, :, pl.ds(k * cap, cap), :], arrived.at[nz + q, :, slots_of(mn), :], V_send.at[q, k - 1], V_recv.at[q, k - 1], node=n
            )

        def lend(q, j):
            return remote(lent.at[q, j], met.at[q, j], x_send.at[q, j], x_recv.at[q, j], local=sibling)

        def deal(q, j):
            to = lax.rem(chip + j, chips) * 2 + core
            return (
                remote(slim.at[q, j - 1], got_slim.at[q, j - 1], q_send.at[q, j - 1], q_recv.at[q, j - 1], local=to),
                remote(thin.at[q, j - 1], got_thin.at[q, j - 1], r_send.at[q, j - 1], r_recv.at[q, j - 1], local=to),
            )

        if npl:
            pl.semaphore_wait(free_up, nn - 1)

        @pl.loop(1, nch)
        def _(t):
            c = chunk_at(t)
            slot = lax.rem(t, RING)
            down_weights(t).wait()

            @pl.loop(0, nl // wide)
            def _(m):
                at = pl.ds(pl.multiple_of(m * step, step), step)
                value = jnp.dot(hid[at, :], dbuf[slot], preferred_element_type=F32)
                sent[c, pl.ds(m * wide, wide)] = value.astype(BF16).reshape(wide, rows, ch)

            @pl.when(t + RING < nch)
            def _():
                down_weights(t + RING).start()

            if npl:
                @pl.when(t <= npl)
                def _():
                    for k in range(1, nn):
                        ascend(t - 1, k).start()

                    @pl.loop(0, nl)
                    def _(l):
                        arrived[c, l, slots_of(mn), :] = sent[c, l, near, :]

            @pl.when(t == nch - 1)
            def _():
                pl.semaphore_wait(free_last, nl - 1)

            @pl.when(t > npl)
            def _():
                for k in range(1, nl):
                    give(c, far, lax.rem(ml + k, nl), p_send, p_recv).start()
                arrived[c, ml] = sent[c, ml]

        @pl.loop(0, nz)
        def _(c):
            for k in range(1, nl):
                give(c, near, lax.rem(ml + k, nl), o_send, o_recv).start()

        @pl.loop(0, nn)
        def _(n):
            mix[n] = mixer(infos[n], mn * nl, 1, nl, topk, cap)

        if npl:
            @pl.loop(0, nl)
            def _(l):
                blur[l] = mixer(peers[l], ml, nl, nn, topk, cap)

        diagonal = lax.broadcasted_iota(jnp.int32, (lines, lines), 0) == lax.broadcasted_iota(jnp.int32, (lines, lines), 1)

        def summed(terms):
            return terms[0:lines] + terms[lines : 2 * lines] + terms[2 * lines : 3 * lines]

        def blend(c, n):
            block = arrived[c, :, slots_of(lax.rem(n - mn + nn, nn)), :].reshape(nl * cap, ch)
            return summed(jnp.dot(mix[n], block, preferred_element_type=F32))

        def pack(value):
            peak = jnp.maximum(jnp.max(jnp.abs(value), axis=1, keepdims=True), 1e-30)
            short = jnp.round(value * (32767.0 / peak)).astype(jnp.int32).astype(I16)
            line = jnp.sum(jnp.where(diagonal, peak, 0.0), axis=0, keepdims=True)
            return short, jnp.broadcast_to(line, (8, lines))

        def unpack(short, line):
            peak = jnp.sum(jnp.where(diagonal, line[0:1, :], 0.0), axis=1, keepdims=True)
            return short.astype(jnp.int32).astype(F32) * (peak * (1.0 / 32767.0))

        def pass_on(c, p, toward, relay):
            work[...] = blend(c, p)

            @pl.when(relay)
            def _():
                land(c, p, toward)
                work[...] += unpack(got[c, p], got_scale[c, p])

            mine = jnp.where(p < mn, p, p - 1)
            part[c, mine], scale[c, mine] = pack(work[...])
            for copy in along(c, p, toward):
                copy.start()

        late = max(nz - 2, 0)

        @pl.loop(0, nz + nn - 2)
        def _(i):
            @pl.when(i < nz)
            def _():
                for k in range(1, nl):
                    take(i, far, k, p_send, p_recv).wait_recv()

            c_up = i - mn
            c_down = i - (nn - 1 - mn)
            for d in reversed(range(nn - 1)):
                @pl.when((c_up >= 0) & (c_up < nz) & (mn + 1 + d < nn))
                def _():
                    pass_on(c_up, mn + 1 + d, 1, mn > 0)

                @pl.when((c_down >= 0) & (c_down < nz) & (mn - 1 - d >= 0))
                def _():
                    pass_on(c_down, mn - 1 - d, -1, mn < nn - 1)

            if npl:
                @pl.when(i == late)
                def _():
                    for q in range(npl):
                        for k in range(1, nn):
                            ascend(q, k).wait_recv()

                        @pl.loop(0, chips)
                        def _(j):
                            to = lax.rem(chip + j, chips) * 2
                            lent[q, j] = summed(
                                jnp.dot(blur[to + 1 - core], arrived[nz + q, to + 1 - core], preferred_element_type=F32)
                            )
                            lend(q, j).start()
                            kept[q, j] = summed(jnp.dot(blur[to + core], arrived[nz + q, to + core], preferred_element_type=F32))

                @pl.when(i == late + 1)
                def _():
                    for q in range(npl):
                        for j in range(chips):
                            lend(q, j).wait_recv()
                            if j:
                                slim[q, j - 1], thin[q, j - 1] = pack(kept[q, j] + met[q, j])
                                for copy in deal(q, j):
                                    copy.start()

        @pl.loop(0, nz)
        def _(c):
            for k in range(1, nl):
                take(c, near, k, o_send, o_recv).wait_recv()
            work[...] = blend(c, mn)

            @pl.when(mn > 0)
            def _():
                land(c, mn, 1)
                work[...] += unpack(got[c, mn], got_scale[c, mn])

            @pl.when(mn < nn - 1)
            def _():
                land(c, nn, -1)
                work[...] += unpack(got[c, nn], got_scale[c, nn])

            out[:, cols(c)] = work[...].astype(out.dtype)

        for q in range(npl):
            total = kept[q, 0] + met[q, 0]
            for j in range(1, chips):
                for copy in deal(q, j):
                    copy.wait_recv()
                total = total + unpack(got_slim[q, j - 1], got_thin[q, j - 1])
            out[:, cols(nz + q)] = total.astype(out.dtype)

        for q in range(npl):
            for k in range(1, nn):
                ascend(q, k).wait_send()
            for j in range(chips):
                lend(q, j).wait_send()
                if j:
                    for copy in deal(q, j):
                        copy.wait_send()

        @pl.loop(0, nz)
        def _(c):
            for k in range(1, nl):
                give(c, far, lax.rem(ml + k, nl), p_send, p_recv).wait_send()
                give(c, near, lax.rem(ml + k, nl), o_send, o_recv).wait_send()
            for d in range(nn - 1):
                @pl.when(mn + 1 + d < nn)
                def _():
                    for copy in along(c, mn + 1 + d, 1):
                        copy.wait_send()

                @pl.when(mn - 1 - d >= 0)
                def _():
                    for copy in along(c, mn - 1 - d, -1):
                        copy.wait_send()


    some, others = max(npl, 1), max(chips - 1, 1)
    pl.run_scoped(
        first_half,
        pltpu.VMEM((nl * rows, 2 * ff), F32),
        pltpu.VMEM((RING, ch, 2 * ff), BF16),
        pltpu.VMEM((nn, nl * cap, lines), BF16),
        pltpu.VMEM((nl, rows, lines), BF16),
    )
    pl.run_scoped(
        second_half,
        pltpu.VMEM((nn, 3 * lines, nl * cap), BF16),
        pltpu.VMEM((nl, 3 * lines, rows), BF16),
        pltpu.VMEM((lines, ch), F32),
        pltpu.VMEM((nz, nn - 1, lines, ch), I16),
        pltpu.VMEM((nz, nn - 1, 8, lines), F32),
        pltpu.VMEM((some, chips, lines, ch), F32),
        pltpu.VMEM((some, chips, lines, ch), F32),
        pltpu.VMEM((some, others, lines, ch), I16),
        pltpu.VMEM((some, others, 8, lines), F32),
    )


def sems(*shape):
    return pltpu.SemaphoreType.DMA(tuple(max(n, 1) for n in shape))


def local(tokens, routes, route_weights, w_gate, w_up, w_down):
    nn, nl = lax.axis_size("node"), lax.axis_size("local")
    exp_dev, width, ff = w_gate.shape
    experts = exp_dev * nn * nl
    assert exp_dev == 1
    lines, topk = routes.shape
    assert topk <= 8
    cap = 4 * lines * topk // (3 * experts)
    rows = nn * cap
    nch = chunks_of(width)
    ch = width // nch
    held_bytes = 2 * lines * width * 3 * nn + 4 * nl * rows * width
    npl = nch // 10 if nl % 2 == 0 and held_bytes <= VMEM_LIMIT * 3 // 4 else 0
    nz = nch - npl
    some = max(npl, 1)
    chips = max(nl // 2, 1)
    others = max(chips - 1, 1)
    spare = 1 if npl == 0 else nl
    wide = -(-experts // 128) * 128

    vmem = pl.BlockSpec(memory_space=pltpu.VMEM)
    hbm = pl.BlockSpec(memory_space=pl.ANY)
    mixed, loss = pl.pallas_call(
        functools.partial(layer_kernel, nn, nl, nch, npl, cap, topk),
        out_shape=(jax.ShapeDtypeStruct((lines, width), tokens.dtype), jax.ShapeDtypeStruct((1, 1), F32)),
        in_specs=[hbm, vmem, vmem, hbm, hbm, hbm],
        out_specs=(vmem, vmem),
        scratch_shapes=[
            pltpu.VMEM((nz, nn, lines, ch), BF16),
            pltpu.VMEM((some, spare, lines, ch), BF16),
            pltpu.VMEM((nch, nl, rows, ch), BF16),
            pltpu.VMEM((nch, nl, rows, ch), BF16),
            pltpu.VMEM((nl * rows, ff), BF16),
            pltpu.VMEM((RING, ff, ch), BF16),
            pltpu.VMEM((nn, 16, lines), F32),
            pltpu.VMEM((nl, 16, lines), F32),
            pltpu.VMEM((nl, 8, wide), F32),
            pltpu.VMEM((8, wide), F32),
            pltpu.VMEM((nz, nn + 1, lines, ch), I16),
            pltpu.VMEM((nz, nn + 1, 8, lines), F32),
            pltpu.VMEM((some, chips if npl else 1, lines, ch), F32),
            pltpu.VMEM((some, others if npl else 1, lines, ch), I16),
            pltpu.VMEM((some, others, 8, lines), F32),
            sems(nz, nn - 1), sems(nz, nn - 1), sems(nz, nn - 1), sems(nz, nn - 1),
            sems(nz, nl - 1), sems(nz, nl - 1),
            sems(some, chips - 1), sems(some, chips - 1), sems(some, chips), sems(some, chips),
            sems(some, nn - 1), sems(some, nn - 1),
            sems(nn - 1), sems(nn - 1), sems(nl - 1), sems(nl - 1), sems(nl - 1), sems(nl - 1),
            sems(nch), sems(RING, 2), sems(RING),
            sems(nz, nl - 1), sems(nz, nl - 1),
            sems(nz, nn - 1), sems(nz, nn + 1), sems(nz, nn - 1), sems(nz, nn + 1),
            sems(some, nn - 1), sems(some, nn - 1), sems(some, chips), sems(some, chips),
            sems(some, chips - 1), sems(some, chips - 1), sems(some, chips - 1), sems(some, chips - 1),
            pltpu.SemaphoreType.REGULAR, pltpu.SemaphoreType.REGULAR, pltpu.SemaphoreType.REGULAR,
        ],
        compiler_params=pltpu.CompilerParams(collective_id=0, has_side_effects=True, vmem_limit_bytes=VMEM_LIMIT),
    )(tokens, routes.T, route_weights.T, w_gate[0], w_up[0], w_down[0])
    return (mixed, loss.reshape(()))


def solution(mesh):
    placed = (
        P(("node", "local"), None),
        P(("node", "local"), None),
        P(("node", "local"), None),
        P(("node", "local"), None, None),
        P(("node", "local"), None, None),
        P(("node", "local"), None, None),
    )
    return jax.shard_map(
        local,
        mesh=mesh,
        in_specs=placed,
        out_specs=(P(("node", "local"), None), P()),
        check_vma=False,
    )
```
